32 devices in a mesh: win: 2 (over core), grp: 16 (over z, y, x).
Axes of the slice: x: 2, y: 2, z: 4, core: 2. Of those that a mesh axis runs over, the one named last changes fastest.
Arguments:
- atom_table: float32 [4, 6, 24576], P('win', None, 'grp'), as said below
- row_blocks: int32 [4, 1024], P('win', 'grp'), may hold values from 0 to 191, as said below
- col_blocks: int32 [4, 1024], P('win', 'grp'), may hold values from 0 to 191, as said below
- lambdas: float32 [4], replicated, may hold values from 0 to 1, as said below
- inverse_temp: float32 [1], replicated, may hold values from 20 to 80
- parity: int32 [1], replicated, may hold values from 0 to 1073741823
- thresholds: int32 [4], replicated, may hold values from 0 to 1073741823
Outputs:
- energies: float32 [4, 3], P('win')
- margins: float32 [4], P('win')
- profile: float32 [4], P('win')
The draws below stay inside these ranges and needn't reach their ends.
Inputs may be any that keep to these rules, and one draw needn't show every extreme that they name: `row_blocks`: the first block of each pair listed on index g of grp lies in that index's share of atoms: blocks g * 12 to (g + 1) * 12 - 1. `col_blocks`: the list of one index of grp names blocks of any one index of grp (itself included) at most 5 times; in each window some index of grp has exactly 5 of its blocks named in every list of that window. `lambdas`: strictly increasing. `atom_table`: field 4 lies in 0.7 to 1.4 and field 5 in 0.6 to 1.4.
All inputs are finite; a program needn't handle non-finite values.
Results may differ from the reference program's by a relative error of at most 0.0003.
Values sent between devices are 32-bit elements; how exact they have to be, the bound alone decides.
A program may use at most 64 MiB of HBM per device.

```python
import math
import jax
import jax.numpy as jnp
from jax import lax

TILE = 128
BLK_DEV = 12
PB_DEV = 64
WINDOWS = 4
BLOCKS = 192
ATOMS = 24576
PAIRS = 1024
SLOTS = 5


def draw_atom_table(key, part):
    keys = jax.random.split(key, 12)
    regions = BLOCKS // BLK_DEV
    centres = jax.random.uniform(keys[0], (WINDOWS, 3, BLOCKS, 1), minval=-1.5, maxval=1.5)
    radius = jnp.exp(jax.random.uniform(keys[1], (WINDOWS, 1, BLOCKS, 1), minval=jnp.log(0.25), maxval=jnp.log(0.9)))
    offsets = jax.random.normal(keys[2], (WINDOWS, 3, BLOCKS, TILE))
    region_charge = 0.3 + 0.6 * jax.random.normal(keys[3], (WINDOWS, regions))
    block_charge = 0.3 * jax.random.normal(keys[4], (WINDOWS, BLOCKS))
    atom_charge = 0.3 * jax.random.normal(keys[5], (WINDOWS, BLOCKS, TILE))
    coords = (centres + radius * offsets).reshape(WINDOWS, 3, ATOMS)
    charge_block = jnp.repeat(region_charge, BLK_DEV, axis=1) + block_charge
    charge = (charge_block[:, :, None] + atom_charge).reshape(WINDOWS, 1, ATOMS)
    depth_block = jnp.exp(jax.random.uniform(keys[6], (WINDOWS, BLOCKS, 1), minval=jnp.log(0.75), maxval=jnp.log(1.3)))
    depth_atom = jnp.exp(jax.random.uniform(keys[7], (WINDOWS, BLOCKS, TILE), minval=jnp.log(0.935), maxval=jnp.log(1.07)))
    depth_root = (depth_block * depth_atom).reshape(WINDOWS, 1, ATOMS)
    size_block = jax.random.uniform(keys[8], (WINDOWS, BLOCKS, 1), minval=0.65, maxval=1.35)
    size_atom = jax.random.uniform(keys[9], (WINDOWS, BLOCKS, TILE), minval=-0.05, maxval=0.05)
    size_sq = (size_block + size_atom).reshape(WINDOWS, 1, ATOMS)
    return jnp.concatenate([coords, charge, depth_root, size_sq], axis=1).astype(jnp.float32)


def draw_row_blocks(key, part):
    offset = jnp.arange(PAIRS, dtype=jnp.int32) // PB_DEV * BLK_DEV
    picks = jax.random.randint(key, (WINDOWS, PAIRS), 0, BLK_DEV, dtype=jnp.int32)
    return picks + offset[None, :]


def draw_col_blocks(key, part):
    groups = PAIRS // PB_DEV
    pool = jnp.arange(groups * SLOTS, dtype=jnp.int32) // SLOTS
    keys = jax.random.split(jax.random.fold_in(key, 7), 2)
    heavy = jax.random.randint(keys[0], (WINDOWS,), 0, groups, dtype=jnp.int32)
    list_keys = jax.random.split(keys[1], WINDOWS * groups)

    def one_list(list_key, heavy_owner):
        first_key, second_key, third_key = jax.random.split(list_key, 3)
        order = jax.random.permutation(first_key, groups * SLOTS)
        owners = pool[order]
        placed = jnp.argsort((owners != heavy_owner).astype(jnp.int32), stable=True)
        chosen = owners[placed][:PB_DEV]
        chosen = jax.random.permutation(second_key, chosen)
        within = jax.random.randint(third_key, (PB_DEV,), 0, BLK_DEV, dtype=jnp.int32)
        return (chosen * BLK_DEV + within).astype(jnp.int32)
    heavy_rows = jnp.repeat(heavy, groups)
    lists = jax.vmap(one_list)(list_keys, heavy_rows)
    return lists.reshape(WINDOWS, PAIRS).astype(jnp.int32)


def draw_lambdas(key, part):
    keys = jax.random.split(jax.random.fold_in(key, 11), 3)
    increments = jax.random.uniform(keys[0], (WINDOWS,), minval=0.5, maxval=1.5)
    start = jax.random.uniform(keys[1], (), minval=0.0, maxval=0.25)
    finish = jax.random.uniform(keys[2], (), minval=0.75, maxval=1.0)
    running = jnp.cumsum(increments)
    unit = (running - running[0]) / (running[-1] - running[0])
    return (start + (finish - start) * unit).astype(jnp.float32)


def plant(drawn, key, least, largest):
    extent = drawn.shape
    place = [jax.random.randint(jax.random.fold_in(key, axis), (), 0, extent[axis]) for axis in range(len(extent))]
    drawn = drawn.at[tuple(place)].set(least)
    longest = extent.index(max(extent))
    place[longest] = (place[longest] + 1) % extent[longest]
    return drawn.at[tuple(place)].set(largest)


def setup_inputs(seed: int = 0) -> dict:
    seeds = jax.random.split(jax.random.key(seed), 8)
    return {
        "atom_table": draw_atom_table(jax.random.fold_in(seeds[7], 71), 0),
        "row_blocks": draw_row_blocks(jax.random.fold_in(seeds[7], 71), 0),
        "col_blocks": draw_col_blocks(jax.random.fold_in(seeds[7], 71), 0),
        "lambdas": draw_lambdas(jax.random.fold_in(seeds[7], 71), 0),
        "inverse_temp": jnp.clip(jnp.exp(jax.random.uniform(seeds[4], (1,), jnp.float32, math.log(20.0), math.log(80.0))), 20.0, 80.0),
        "parity": jax.random.randint(seeds[5], (1,), 0, 1073741824).astype(jnp.int32),
        "thresholds": plant(jax.random.randint(seeds[6], (WINDOWS,), 0, 1073741824), jax.random.fold_in(seeds[6], 1), 0, 1073741823).astype(jnp.int32),
    }


tiles_per_step = 16

def pair_energy(row_data, col_data, same_block, lambda_set):
    delta_x = row_data[0][:, :, None] - col_data[0][:, None, :]
    delta_y = row_data[1][:, :, None] - col_data[1][:, None, :]
    delta_z = row_data[2][:, :, None] - col_data[2][:, None, :]
    distance = delta_x * delta_x + delta_y * delta_y + delta_z * delta_z
    charge_pair = row_data[3][:, :, None] * col_data[3][:, None, :]
    well_depth = 4.0 * row_data[4][:, :, None] * col_data[4][:, None, :]
    size_pair = row_data[5][:, :, None] * col_data[5][:, None, :]
    scaled = distance / size_pair
    scaled_cube = scaled * scaled * scaled
    width_tile = distance.shape[-1]
    diagonal = (lax.broadcasted_iota(jnp.int32, (width_tile, width_tile), 0) == lax.broadcasted_iota(jnp.int32, (width_tile, width_tile), 1)).astype(jnp.float32)
    keep_mask = 1.0 - same_block[:, None, None] * diagonal[None]
    totals = []
    for number in range(3):
        lam_now = lambda_set[number]
        softened = 1.0 - 0.5 * lam_now + scaled_cube
        inverse = 1.0 / softened
        dispersion = well_depth * (inverse * inverse - inverse)
        coulomb = charge_pair * lax.rsqrt(distance + 2.0 - lam_now)
        totals.append(lam_now * jnp.sum(keep_mask * (dispersion + coulomb)))
    return jnp.stack(totals)

def window_sums(table, row_ids, col_ids, lambda_set):
    blocks = table.reshape(table.shape[0], -1, TILE)
    row_all = jnp.take(blocks, row_ids, axis=1)
    col_all = jnp.take(blocks, col_ids, axis=1)
    same_all = (row_ids == col_ids).astype(jnp.float32)
    count = row_ids.shape[0] // tiles_per_step

    def advance(number, total):
        start = number * tiles_per_step
        row_part = lax.dynamic_slice_in_dim(row_all, start, tiles_per_step, 1)
        col_part = lax.dynamic_slice_in_dim(col_all, start, tiles_per_step, 1)
        same_part = lax.dynamic_slice_in_dim(same_all, start, tiles_per_step, 0)
        return total + pair_energy(row_part, col_part, same_part, lambda_set)
    return lax.fori_loop(0, count, advance, jnp.zeros((3,), jnp.float32))

def reference(atom_table, row_blocks, col_blocks, lambdas, inverse_temp, parity, thresholds):
    windows = lambdas.shape[0]
    window = jnp.arange(windows, dtype=jnp.int32)
    below = jnp.clip(window - 1, 0, windows - 1)
    above = jnp.clip(window + 1, 0, windows - 1)
    lambda_sets = jnp.stack([lambdas[below], lambdas, lambdas[above]], axis=1)
    sums = lax.map(lambda pack: window_sums(pack[0], pack[1], pack[2], pack[3]), (atom_table, row_blocks, col_blocks, lambda_sets))
    energies = sums / (row_blocks.shape[1] * TILE * TILE)
    d_plus = energies[:, 2] - energies[:, 1]
    d_minus = energies[:, 0] - energies[:, 1]
    profile = jnp.concatenate([jnp.zeros((1,), jnp.float32), jnp.cumsum(d_plus)[:-1]])
    lower_win = jnp.where(jnp.remainder(window - parity[0], 2) == 0, window, window - 1)
    upper_win = lower_win + 1
    has_partner = (lower_win >= 0) & (upper_win < windows)
    lower_safe = jnp.clip(lower_win, 0, windows - 1)
    upper_safe = jnp.clip(upper_win, 0, windows - 1)
    change = d_plus[lower_safe] + d_minus[upper_safe]
    offset_draw = jnp.remainder(thresholds[lower_safe] + parity[0], 1073741824).astype(jnp.int32) + 1
    draw_share = offset_draw.astype(jnp.float32) / 1073741824.0
    margins = jnp.where(has_partner, -jnp.log(draw_share) - inverse_temp[0] * change, 0.0)
    return (energies, margins, profile)
```

```python
import functools

import jax
import jax.numpy as jnp
from jax import lax
from jax.experimental import pallas as pl
from jax.experimental.pallas import tpu as pltpu
from jax.sharding import PartitionSpec as P

TILE = 128
ROWS = 8
FIELDS = 6
PIECES = TILE // ROWS
UNROLL = 4
LIMIT = 48 * 1024 * 1024
MESH = pl.DeviceIdType.MESH


def grid_of(mesh):
    groups = mesh.shape["grp"]
    try:
        line = mesh.devices[0]
        coords = [tuple(d.coords) for d in line]
        dims = [len({c[a] for c in coords}) for a in (2, 1, 0)]
        base = [min(c[a] for c in coords) for a in (2, 1, 0)]
        want = [
            (base[2] + x, base[1] + y, base[0] + z)
            for z in range(dims[0])
            for y in range(dims[1])
            for x in range(dims[2])
        ]
        if [c[:3] for c in coords] == want:
            return tuple(dims)
    except Exception:
        pass
    return (groups, 1, 1)


def messages_of(dims):
    z, y, x = dims
    first = (z - 1) + (x - 1) + (y - 1)
    second = (z - 1) * (x + y - 2)
    third = z * (x - 1) * (y - 1)
    return first + second + third


def split3(value):
    high = value.astype(jnp.bfloat16).astype(jnp.float32)
    rest = value - high
    middle = rest.astype(jnp.bfloat16).astype(jnp.float32)
    return high, middle, rest - middle


def kernel(
    cfg,
    table,
    row_hbm,
    col_hbm,
    lambdas_hbm,
    inverse_temp,
    parity,
    thresholds_hbm,
    out,
    *scratch,
):
    run, wins, groups, own, listed, dims = cfg
    bufs = scratch[:run]
    rowbs = scratch[run : 2 * run]
    (
        stage,
        feats,
        red,
        row_ids,
        col_ids,
        lambdas,
        thresholds,
        load_sem,
        small_sem,
        send_sem,
        recv_sem,
        red_send,
        red_recv,
        ready,
    ) = scratch[2 * run :]
    dim_z, dim_y, dim_x = dims
    windows = wins * run
    win = lax.axis_index("win")
    grp = lax.axis_index("grp")
    my_z = grp // (dim_y * dim_x)
    my_y = (grp // dim_x) % dim_y
    my_x = grp % dim_x
    two_ends = wins == 2 and run == 2
    own_pad = stage.shape[2]
    me = win * groups + grp

    def window_of(slot):
        if two_ends:
            return jnp.where(win == 0, 1 - slot, slot)
        return slot

    def lams_of(slot):
        return 2 if two_ends and slot == 1 else 3

    def fields_of(slot):
        return FIELDS + lams_of(slot)

    def group_at(z, dy, dx):
        return (z * dim_y + (my_y + dy) % dim_y) * dim_x + (my_x + dx) % dim_x

    def plane_at(step):
        places = [
            sorted(range(dim_z), key=lambda z: (abs(z - mine), z))[step]
            for mine in range(dim_z)
        ]
        chosen = places[0]
        for mine in range(1, dim_z):
            chosen = jnp.where(my_z == mine, places[mine], chosen)
        return chosen

    planes = [my_z] + [plane_at(step) for step in range(1, dim_z)]

    loads = []
    for slot in range(run):
        local = window_of(slot)
        for f in range(FIELDS):
            loads.append(
                pltpu.make_async_copy(
                    table.at[f, :, local, :],
                    bufs[slot].at[pl.ds(grp * own, own), f, 0, :],
                    load_sem.at[slot],
                )
            )
    for slot in range(run):
        local = window_of(slot)
        loads.append(
            pltpu.make_async_copy(
                table.at[:, :, local, :],
                stage.at[slot, :, pl.ds(0, own), :],
                load_sem.at[run + slot],
            )
        )
    smalls = [
        pltpu.make_async_copy(row_hbm, row_ids, small_sem.at[0]),
        pltpu.make_async_copy(col_hbm, col_ids, small_sem.at[1]),
        pltpu.make_async_copy(lambdas_hbm, lambdas, small_sem.at[2]),
        pltpu.make_async_copy(thresholds_hbm, thresholds, small_sem.at[3]),
    ]
    for copy in loads:
        copy.start()
    for copy in smalls:
        copy.start()

    barrier = pltpu.get_barrier_semaphore()
    partners = [((win + step) % wins, grp) for step in range(1, wins)]
    peers = [(win, group_at(plane, 0, 0)) for plane in planes[1:]]
    peers += [(win, group_at(my_z, 0, dx)) for dx in range(1, dim_x)]
    peers += [(win, group_at(my_z, dy, 0)) for dy in range(1, dim_y)]
    peers += partners
    for peer in peers:
        pl.semaphore_signal(barrier, inc=1, device_id=peer, device_id_type=MESH)

    for copy in smalls:
        copy.wait()

    def lambda_list(slot):
        window = win * run + window_of(slot)
        if two_ends and slot == 1:
            low = jnp.where(window == 0, 0, window - 1)
            return [lambdas[low], lambdas[low + 1]]
        return [
            lambdas[jnp.maximum(window - 1, 0)],
            lambdas[window],
            lambdas[jnp.minimum(window + 1, windows - 1)],
        ]

    for copy in loads:
        copy.wait()

    pl.semaphore_wait(barrier, len(peers))

    counts = [0] * run

    def share_of(slot, owner):
        return bufs[slot].at[pl.ds(owner * own, own)]

    def descriptor(slot, owner, target, number):
        return pltpu.make_async_remote_copy(
            src_ref=share_of(slot, owner),
            dst_ref=share_of(slot, owner),
            send_sem=send_sem.at[slot, number],
            recv_sem=recv_sem.at[slot, owner],
            device_id={"grp": target},
            device_id_type=MESH,
        )

    sent = []

    def send(slot, owner, target):
        copy = descriptor(slot, owner, target, counts[slot])
        counts[slot] += 1
        copy.start()
        sent.append(copy)

    def arrived(slot, owner):
        descriptor(slot, owner, owner, 0).wait_recv()

    def to_x(slot, owner):
        for dx in range(1, dim_x):
            send(slot, owner, group_at(my_z, 0, dx))

    def to_y(slot, owner):
        for dy in range(1, dim_y):
            send(slot, owner, group_at(my_z, dy, 0))

    def open_sends(slot):
        for plane in planes[1:]:
            send(slot, grp, group_at(plane, 0, 0))
        to_x(slot, grp)
        to_y(slot, grp)

    def pass_column(slot, step):
        owner = group_at(planes[step], 0, 0)
        arrived(slot, owner)
        to_x(slot, owner)
        to_y(slot, owner)

    def pass_plane(slot, step):
        for dx in range(1, dim_x):
            owner = group_at(planes[step], 0, dx)
            arrived(slot, owner)
            if step % 2 == 0:
                to_y(slot, owner)
        for dy in range(1, dim_y):
            owner = group_at(planes[step], dy, 0)
            arrived(slot, owner)
            if step % 2 == 1:
                to_x(slot, owner)

    def last_arrivals(slot):
        for step in range(dim_z):
            for dy in range(1, dim_y):
                for dx in range(1, dim_x):
                    arrived(slot, group_at(planes[step], dy, dx))

    def spread(slot):
        lams = lambda_list(slot)
        count = fields_of(slot)
        depth = stage[slot, 4]
        inverse_root = lax.rsqrt(depth)
        sixth = jnp.exp(jnp.log(depth) * (-1.0 / 6.0))
        values = [stage[slot, f] for f in range(4)]
        values += [depth * inverse_root, sixth / stage[slot, 5]]
        values += [inverse_root * (1.0 - 0.5 * lam) for lam in lams]
        for f, value in enumerate(values):
            for part, piece in enumerate(split3(value)):
                feats[pl.ds((part * count + f) * own_pad, own_pad), :] = piece
        for row in range(3 * count, 32):
            feats[pl.ds(row * own_pad, own_pad), :] = jnp.zeros((own_pad, TILE), jnp.float32)
        source = lax.broadcasted_iota(jnp.int32, (32, count * TILE), 0)
        target = lax.broadcasted_iota(jnp.int32, (32, count * TILE), 1) // TILE
        picks = jnp.zeros((32, count * TILE), jnp.float32)
        for part in range(3):
            picks = jnp.where(source == target + part * count, 1.0, picks)
        picks = picks.astype(jnp.bfloat16)

        def one(block, carry):
            lines = feats[pl.ds(block, 32, stride=own_pad), :].astype(jnp.bfloat16)
            wide = lax.dot_general(
                lines, picks, (((0,), (0,)), ((), ())), preferred_element_type=jnp.float32
            )
            for f in range(count):
                for piece in range(PIECES):
                    rowbs[slot][(block * count + f) * PIECES + piece] = wide[
                        piece * ROWS : (piece + 1) * ROWS, f * TILE : (f + 1) * TILE
                    ]
            return carry

        lax.fori_loop(0, own, one, 0)

    def start_state(slot):
        zero = jnp.zeros((ROWS, TILE), jnp.float32)
        row = jnp.zeros((1, TILE), jnp.float32)
        return tuple(zero for _ in range(lams_of(slot))) + (row, row)

    def tiles(slot, first, last, state):
        local = window_of(slot)
        lams = lambda_list(slot)
        softs = [2.0 - lam for lam in lams]
        base = grp * own
        count = fields_of(slot)
        unroll = UNROLL if listed % UNROLL == 0 else 1

        def pair_sum(pair, state):
            row_id = row_ids[local, pair]
            col_id = col_ids[local, pair]
            col = [bufs[slot][col_id, f] for f in range(FIELDS)]
            mine = jnp.clip(row_id - base, 0, own - 1) * (count * PIECES)
            fields = [jnp.broadcast_to(col[f], (ROWS, TILE)) for f in range(3)]
            charge_col = col[3]
            depth_col = col[4]
            size_col = jnp.broadcast_to(1.0 / col[5], (ROWS, TILE))
            sum_disp = [None] * len(lams)
            sum_coul = [None] * len(lams)
            for piece in range(PIECES):
                wide = [rowbs[slot][mine + (f * PIECES + piece)] for f in range(count)]
                dx = wide[0] - fields[0]
                dy = wide[1] - fields[1]
                dz = wide[2] - fields[2]
                r2 = dx * dx + dy * dy + dz * dz
                scaled = r2 * (wide[5] * size_col)
                cube = scaled * scaled * scaled
                for k in range(len(lams)):
                    inverse = 1.0 / (cube + wide[FIELDS + k])
                    disp = inverse * (inverse - wide[4])
                    coul = wide[3] * lax.rsqrt(r2 + softs[k])
                    if piece == 0:
                        sum_disp[k], sum_coul[k] = disp, coul
                    else:
                        sum_disp[k] = sum_disp[k] + disp
                        sum_coul[k] = sum_coul[k] + coul
            depth_four = 4.0 * depth_col
            totals = [
                state[k] + (sum_disp[k] * depth_four + sum_coul[k] * charge_col)
                for k in range(len(lams))
            ]
            same = jnp.where(row_id == col_id, 1.0, 0.0)
            return tuple(totals) + (
                state[-2] + same * (depth_col * depth_col),
                state[-1] + same * (charge_col * charge_col),
            )

        def some(step, state):
            for part in range(unroll):
                state = pair_sum(step * unroll + part, state)
            return state

        return lax.fori_loop(first // unroll, last // unroll, some, state)

    def close(slot, state):
        sums = []
        for k, lam in enumerate(lambda_list(slot)):
            core = jnp.full((1, TILE), 1.0 - 0.5 * lam, jnp.float32)
            soft = jnp.full((1, TILE), 2.0 - lam, jnp.float32)
            inverse = 1.0 / core
            own_pairs = state[-2] * (4.0 * inverse * (inverse - 1.0)) + state[-1] * lax.rsqrt(soft)
            line = jnp.sum(state[k], axis=0, keepdims=True) - own_pairs
            sums.append(jnp.sum(line, axis=1, keepdims=True) * lam)
        if two_ends and slot == 1:
            sums = [sums[0], jnp.where(win == 0, sums[0], sums[1]), sums[1]]
        return sums

    for slot in range(run):
        open_sends(slot)
    for slot in range(run):
        spread(slot)

    shares = []
    lowers = []
    for wl in range(run):
        window = win * run + wl
        odd = (window + parity[0]) & 1
        lower = window - odd
        threshold = thresholds[0]
        for v in range(1, windows):
            threshold = jnp.where(lower == v, thresholds[v], threshold)
        drawn = ((threshold + parity[0]) & 1073741823) + 1
        share = jnp.full((ROWS, TILE), drawn, jnp.int32).astype(jnp.float32) * (1.0 / 1073741824.0)
        shares.append(-jnp.log(share))
        lowers.append(lower)

    for step in range(1, dim_z):
        pass_column(0, step)
        if step == 1:
            pass_plane(0, 0)
    for step in range(1, dim_z):
        pass_plane(0, step)
    if dim_z == 1:
        pass_plane(0, 0)
    if run > 1:
        for step in range(1, dim_z):
            pass_column(1, step)
    last_arrivals(0)
    for partner in partners:
        pl.semaphore_signal(ready, inc=1, device_id=partner, device_id_type=MESH)

    partial = []
    for slot in range(run):
        state = start_state(slot)
        first = 0
        if slot + 1 < run:
            if slot > 0:
                for step in range(1, dim_z):
                    pass_column(slot + 1, step)
            for step in range(dim_z):
                until = listed * (step + 1) // (2 * dim_z) // UNROLL * UNROLL
                state = tiles(slot, first, until, state)
                first = until
                pass_plane(slot + 1, step)
        state = tiles(slot, first, listed, state)
        if slot + 1 < run:
            last_arrivals(slot + 1)
        partial.append(close(slot, state))

    lane = lax.broadcasted_iota(jnp.int32, (1, TILE), 1)
    line = jnp.zeros((1, TILE), jnp.float32)
    for slot in range(run):
        place = (win * run + window_of(slot)) * 3
        for k in range(3):
            line = jnp.where(lane == place + k, partial[slot][k], line)
    red[me] = line
    for _ in partners:
        pl.semaphore_wait(ready, 1)
    everyone = wins * groups
    for other_win in range(wins):
        for step in range(groups):
            if other_win or step:
                target = ((win + other_win) % wins, (grp + step) % groups)
                pltpu.make_async_remote_copy(
                    src_ref=red.at[me],
                    dst_ref=red.at[me],
                    send_sem=red_send.at[0],
                    recv_sem=red_recv.at[0],
                    device_id=target,
                    device_id_type=MESH,
                ).start()
    for copy in sent:
        copy.wait_send()
    rest = pltpu.make_async_remote_copy(
        src_ref=red.at[pl.ds(0, everyone - 1)],
        dst_ref=red.at[pl.ds(0, everyone - 1)],
        send_sem=red_send.at[0],
        recv_sem=red_recv.at[0],
        device_id=((win + 1) % wins, (grp + 1) % groups),
        device_id_type=MESH,
    )
    rest.wait_recv()
    rest.wait_send()
    scale = 1.0 / (listed * groups * TILE * TILE)
    total = jnp.sum(red[0:everyone], axis=0) * scale
    energy = [
        [jnp.sum(jnp.where(lane == v * 3 + k, total, 0.0)) for k in range(3)]
        for v in range(windows)
    ]
    ups = [e[2] - e[1] for e in energy]
    downs = [e[0] - e[1] for e in energy]
    rows = lax.broadcasted_iota(jnp.int32, (ROWS, TILE), 0)
    lanes = lax.broadcasted_iota(jnp.int32, (ROWS, TILE), 1)
    cell = rows * TILE + lanes
    result = jnp.zeros((ROWS, TILE), jnp.float32)
    for wl in range(run):
        window = win * run + wl
        for k in range(3):
            value = energy[wl][k]
            for part in range(1, wins):
                value = jnp.where(win == part, energy[part * run + wl][k], value)
            result = jnp.where(cell == wl * TILE + k, value, result)
        profile = jnp.float32(0.0)
        change = jnp.float32(0.0)
        for v in range(windows):
            profile = profile + jnp.where(v < window, ups[v], 0.0)
            change = change + jnp.where(lowers[wl] == v, ups[v], 0.0)
            change = change + jnp.where(lowers[wl] + 1 == v, downs[v], 0.0)
        result = jnp.where(cell == (run + 1) * TILE + wl, profile, result)
        partner = jnp.logical_and(lowers[wl] >= 0, lowers[wl] + 1 < windows)
        margin = shares[wl] - inverse_temp[0] * change
        margin = jnp.where(partner, margin, 0.0)
        result = jnp.where(cell == run * TILE + wl, margin, result)
    out[...] = result


def finish(run, total, out_energy, out_margin, out_profile):
    out_energy[...] = total[0:run, 0:3]
    out_margin[...] = total[run, 0:run]
    out_profile[...] = total[run + 1, 0:run]


def per_device(dims, atom_table, row_blocks, col_blocks, lambdas, inverse_temp, parity, thresholds):
    run, fields, atoms = atom_table.shape
    wins = lax.axis_size("win")
    groups = lax.axis_size("grp")
    own = atoms // TILE
    listed = row_blocks.shape[1]
    cfg = (run, wins, groups, own, listed, dims)
    hbm = pl.BlockSpec(memory_space=pltpu.HBM)
    vmem = pl.BlockSpec(memory_space=pltpu.VMEM)
    smem = pl.BlockSpec(memory_space=pltpu.SMEM)
    own_pad = -(-own // 8) * 8
    counts = [9] * run
    if wins == 2 and run == 2:
        counts[1] = 8
    scratch = [pltpu.VMEM((groups * own, FIELDS, 1, TILE), jnp.float32) for _ in range(run)]
    scratch += [pltpu.VMEM((own * count * PIECES, ROWS, TILE), jnp.float32) for count in counts]
    scratch += [
        pltpu.VMEM((run, FIELDS, own_pad, TILE), jnp.float32),
        pltpu.VMEM((32 * own_pad, TILE), jnp.float32),
        pltpu.VMEM((wins * groups, 1, TILE), jnp.float32),
        pltpu.SMEM((run, listed), jnp.int32),
        pltpu.SMEM((run, listed), jnp.int32),
        pltpu.SMEM((wins * run,), jnp.float32),
        pltpu.SMEM((wins * run,), jnp.int32),
        pltpu.SemaphoreType.DMA((2 * run,)),
        pltpu.SemaphoreType.DMA((4,)),
        pltpu.SemaphoreType.DMA((run, max(1, messages_of(dims)))),
        pltpu.SemaphoreType.DMA((run, groups)),
        pltpu.SemaphoreType.DMA((1,)),
        pltpu.SemaphoreType.DMA((1,)),
        pltpu.SemaphoreType.REGULAR,
    ]
    table = jnp.transpose(atom_table.reshape(run, fields, own, TILE), (1, 2, 0, 3))
    total = pl.pallas_call(
        functools.partial(kernel, cfg),
        out_shape=jax.ShapeDtypeStruct((8, TILE), jnp.float32),
        in_specs=[hbm, hbm, hbm, hbm, smem, smem, hbm],
        out_specs=vmem,
        scratch_shapes=scratch,
        compiler_params=pltpu.CompilerParams(
            collective_id=0, has_side_effects=True, vmem_limit_bytes=LIMIT
        ),
    )(table, row_blocks, col_blocks, lambdas, inverse_temp, parity, thresholds)
    shapes = (
        jax.ShapeDtypeStruct((run, 3), jnp.float32),
        jax.ShapeDtypeStruct((run,), jnp.float32),
        jax.ShapeDtypeStruct((run,), jnp.float32),
    )
    return pl.pallas_call(
        functools.partial(finish, run),
        out_shape=shapes,
        in_specs=[vmem],
        out_specs=(vmem, vmem, vmem),
        compiler_params=pltpu.CompilerParams(vmem_limit_bytes=1024 * 1024),
    )(total)


def solution(mesh):
    return jax.shard_map(
        functools.partial(per_device, grid_of(mesh)),
        mesh=mesh,
        in_specs=(P("win", None, "grp"), P("win", "grp"), P("win", "grp"), P(), P(), P(), P()),
        out_specs=(P("win", None), P("win"), P("win")),
        check_vma=False,
    )
```

```python
import functools

import jax
import jax.numpy as jnp
from jax import lax
from jax.experimental import pallas as pl
from jax.experimental.pallas import tpu as pltpu
from jax.sharding import PartitionSpec as P

TILE = 128
ROWS = 8
FIELDS = 6
PIECES = TILE // ROWS
UNROLL = 4
SPREAD = 4
DIRECT = {(0, 0), (0, 1), (0, 2), (0, 3), (1, 2), (1, 3)}
LINES = 40
LIMIT = 67043328
MESH = pl.DeviceIdType.MESH


def grid_of(mesh):
    groups = mesh.shape["grp"]
    try:
        line = mesh.devices[0]
        coords = [tuple(d.coords) for d in line]
        dims = [len({c[a] for c in coords}) for a in (2, 1, 0)]
        base = [min(c[a] for c in coords) for a in (2, 1, 0)]
        want = [
            (base[2] + x, base[1] + y, base[0] + z)
            for z in range(dims[0])
            for y in range(dims[1])
            for x in range(dims[2])
        ]
        if [c[:3] for c in coords] == want:
            return tuple(dims)
    except Exception:
        pass
    return (groups, 1, 1)


def messages_of(dims):
    z, y, x = dims
    return (z - 1) + z * (x * y - 1)


def near_steps(dims):
    return min(2, dims[0])


def phases_of(dims, groups, listed):
    z, y, x = dims
    slots = listed // groups + 1
    ends = []
    for step in range(near_steps(dims), z + 1):
        ends.append(max(0, listed - slots * (z - step) * y * x))
    return ends


def bits_for(count):
    return max(1, (count - 1).bit_length())


def split3(value):
    high = value.astype(jnp.bfloat16).astype(jnp.float32)
    rest = value - high
    middle = rest.astype(jnp.bfloat16).astype(jnp.float32)
    return high, middle, rest - middle


def kernel(
    cfg,
    table,
    row_hbm,
    col_hbm,
    lambdas_hbm,
    inverse_temp,
    parity,
    thresholds_hbm,
    out,
    *scratch,
):
    run, wins, groups, own, listed, dims = cfg
    dim_z, dim_y, dim_x = dims
    near = near_steps(dims)
    parts = dim_z - near + 1
    bufs = [scratch[slot * parts : (slot + 1) * parts] for slot in range(run)]
    scratch = scratch[run * parts :]
    rowbs = scratch[:run]
    (
        stage,
        feats,
        red,
        row_ids,
        col_ids,
        words,
        order,
        lambdas,
        thresholds,
        load_sem,
        small_sem,
        send_sem,
        recv_sem,
        red_send,
        red_recv,
        ready,
        order_sem,
    ) = scratch[run:]
    windows = wins * run
    win = lax.axis_index("win")
    grp = lax.axis_index("grp")
    my_z = grp // (dim_y * dim_x)
    my_y = (grp // dim_x) % dim_y
    my_x = grp % dim_x
    two_ends = wins == 2 and run == 2
    own_pad = stage.shape[2]
    me = win * groups + grp

    def window_of(slot):
        if two_ends:
            return jnp.where(win == 0, 1 - slot, slot)
        return slot

    def lams_of(slot):
        return 2 if two_ends and slot == 1 else 3

    def fields_of(slot):
        return FIELDS + lams_of(slot)

    plane = dim_y * dim_x
    span = plane * own
    row_bits = bits_for(own)
    index_bits = bits_for(near * span)

    def group_at(z, dy, dx):
        return (z * dim_y + (my_y + dy) % dim_y) * dim_x + (my_x + dx) % dim_x

    def place_at(dy, dx):
        return ((my_y + dy) % dim_y) * dim_x + (my_x + dx) % dim_x

    paired = dim_z & (dim_z - 1) == 0

    def flipped(step):
        other = 0
        for bit in range(bits_for(dim_z)):
            mine = (my_z // 2**bit) % 2
            other = other + 2**bit * ((1 - mine) if (step >> bit) & 1 else mine)
        return other

    def plane_to(step):
        return flipped(step) if paired else (my_z + step) % dim_z

    def plane_from(step):
        return flipped(step) if paired else (my_z - step + dim_z) % dim_z

    def share_of(slot, step, place):
        if step < near:
            return bufs[slot][0].at[pl.ds((step * plane + place) * own, own)]
        return bufs[slot][step - near + 1].at[pl.ds(place * own, own)]

    my_place = place_at(0, 0)
    others = [(dy, dx) for dy in range(dim_y) for dx in range(dim_x) if dy or dx]

    loads = []
    for slot in range(run):
        local = window_of(slot)
        for f in range(FIELDS):
            loads.append(
                pltpu.make_async_copy(
                    table.at[f, :, local, :],
                    bufs[slot][0].at[pl.ds(my_place * own, own), f, 0, :],
                    load_sem.at[slot],
                )
            )
    for slot in range(run):
        local = window_of(slot)
        loads.append(
            pltpu.make_async_copy(
                table.at[:, :, local, :],
                stage.at[slot, :, pl.ds(0, own), :],
                load_sem.at[run + slot],
            )
        )
    smalls = [
        pltpu.make_async_copy(row_hbm, row_ids, small_sem.at[0]),
        pltpu.make_async_copy(col_hbm, col_ids, small_sem.at[1]),
        pltpu.make_async_copy(lambdas_hbm, lambdas, small_sem.at[2]),
        pltpu.make_async_copy(thresholds_hbm, thresholds, small_sem.at[3]),
    ]
    for copy in loads:
        copy.start()
    for copy in smalls:
        copy.start()

    barrier = pltpu.get_barrier_semaphore()
    partners = [((win + step) % wins, grp) for step in range(1, wins)]
    peers = [(win, group_at(plane_to(step), 0, 0)) for step in range(1, dim_z)]
    peers += [(win, group_at(my_z, dy, dx)) for dy, dx in others]
    peers += partners
    for peer in peers:
        pl.semaphore_signal(barrier, inc=1, device_id=peer, device_id_type=MESH)

    for copy in smalls:
        copy.wait()

    def lambda_list(slot):
        window = win * run + window_of(slot)
        if two_ends and slot == 1:
            low = jnp.where(window == 0, 0, window - 1)
            return [lambdas[low], lambdas[low + 1]]
        return [
            lambdas[jnp.maximum(window - 1, 0)],
            lambdas[window],
            lambdas[jnp.minimum(window + 1, windows - 1)],
        ]

    def sort_pairs(slot):
        local = window_of(slot)
        rows = row_ids[pl.ds(local, 1), :]
        cols = col_ids[pl.ds(local, 1), :]
        zone = jnp.zeros((1, listed), jnp.int32)
        for z in range(1, dim_z):
            zone = zone + jnp.where(cols >= z * span, 1, 0)
        step_of = jnp.zeros((1, listed), jnp.int32)
        for step in range(1, dim_z):
            step_of = jnp.where(zone == plane_from(step), step, step_of)
        index = cols - zone * span
        index = index + jnp.where(step_of < near, step_of, 0) * span
        mine = jnp.clip(rows - grp * own, 0, own - 1)
        word = (step_of * 2**index_bits + index) * 2**row_bits + mine
        word = word * 2 + jnp.where(rows == cols, 1, 0)
        lane = lax.broadcasted_iota(jnp.int32, (listed, listed), 1)
        line = lax.broadcasted_iota(jnp.int32, (listed, listed), 0)
        eye = lane == line
        rank = step_of * listed + lax.broadcasted_iota(jnp.int32, (1, listed), 1)
        rank_row = jnp.broadcast_to(rank.astype(jnp.float32), (listed, listed))
        word_row = jnp.broadcast_to(word.astype(jnp.float32), (listed, listed))
        rank_col = jnp.sum(jnp.where(eye, rank_row, 0.0), axis=1, keepdims=True)
        word_col = jnp.sum(jnp.where(eye, word_row, 0.0), axis=1, keepdims=True)
        spot = jnp.sum(jnp.where(rank_row < rank_col, 1.0, 0.0), axis=1, keepdims=True)
        hit = spot == lane.astype(jnp.float32)
        sorted_row = jnp.sum(jnp.where(hit, word_col, 0.0), axis=0, keepdims=True)
        words[pl.ds(slot, 1), :] = sorted_row.astype(jnp.int32)

    for copy in loads:
        copy.wait()

    pl.semaphore_wait(barrier, len(peers))

    counts = [0] * run
    sent = []

    def descriptor(slot, source, target_at, peer, number):
        return pltpu.make_async_remote_copy(
            src_ref=share_of(slot, *source),
            dst_ref=share_of(slot, *target_at),
            send_sem=send_sem.at[slot, number],
            recv_sem=recv_sem.at[slot, target_at[0], target_at[1]],
            device_id={"grp": peer},
            device_id_type=MESH,
        )

    def send(slot, source, target_at, peer):
        copy = descriptor(slot, source, target_at, peer, counts[slot])
        counts[slot] += 1
        copy.start()
        sent.append(copy)

    def arrived(slot, step, place):
        at = (step, place)
        descriptor(slot, at, at, grp, 0).wait_recv()

    def to_plane(slot, step, place, dy, dx):
        send(slot, (step, place), (step, place), group_at(my_z, dy, dx))

    def to_direct(slot, step):
        for dy, dx in others:
            if (slot, step) in DIRECT or dy == 0 or dx == 0:
                to_plane(slot, step, my_place, dy, dx)

    def open_sends(slot):
        for step in range(1, dim_z):
            send(slot, (0, my_place), (step, my_place), group_at(plane_to(step), 0, 0))
        to_direct(slot, 0)

    def pass_column(slot, step):
        arrived(slot, step, my_place)
        to_direct(slot, step)

    def pass_plane(slot, step):
        for dx in range(1, dim_x):
            arrived(slot, step, place_at(0, dx))
            if (slot, step) not in DIRECT and step % 2 == 0:
                for dy in range(1, dim_y):
                    to_plane(slot, step, place_at(0, dx), dy, 0)
        for dy in range(1, dim_y):
            arrived(slot, step, place_at(dy, 0))
            if (slot, step) not in DIRECT and step % 2 == 1:
                for dx in range(1, dim_x):
                    to_plane(slot, step, place_at(dy, 0), 0, dx)

    def last_arrivals(slot, step):
        for dy in range(1, dim_y):
            for dx in range(1, dim_x):
                arrived(slot, step, place_at(dy, dx))

    def spread(slot):
        lams = lambda_list(slot)
        count = fields_of(slot)
        depth = stage[slot, 4]
        inverse_root = lax.rsqrt(depth)
        sixth = jnp.exp(jnp.log(depth) * (-1.0 / 6.0))
        values = [stage[slot, f] for f in range(4)]
        values += [depth * inverse_root, sixth / stage[slot, 5]]
        values += [inverse_root * (1.0 - 0.5 * lam) for lam in lams]
        for f, value in enumerate(values):
            for part, piece in enumerate(split3(value)):
                feats[pl.ds(part * count + f, own_pad, stride=LINES), :] = piece
        for row in range(3 * count, 32):
            feats[pl.ds(row, own_pad, stride=LINES), :] = jnp.zeros((own_pad, TILE), jnp.float32)
        source = lax.broadcasted_iota(jnp.int32, (32, count * TILE), 0)
        target = lax.broadcasted_iota(jnp.int32, (32, count * TILE), 1) // TILE
        picks = jnp.zeros((32, count * TILE), jnp.float32)
        for part in range(3):
            picks = jnp.where(source == target + part * count, 1.0, picks)
        picks = picks.astype(jnp.bfloat16)

        def one(block):
            start = pl.multiple_of(block * LINES, 8)
            lines = feats[pl.ds(start, 32), :].astype(jnp.bfloat16)
            wide = lax.dot_general(
                lines, picks, (((0,), (0,)), ((), ())), preferred_element_type=jnp.float32
            )
            for f in range(count):
                for piece in range(PIECES):
                    rowbs[slot][(block * count + f) * PIECES + piece] = wide[
                        piece * ROWS : (piece + 1) * ROWS, f * TILE : (f + 1) * TILE
                    ]

        def some(step, carry):
            for part in range(together):
                one(step * together + part)
            return carry

        together = SPREAD if own % SPREAD == 0 else 1
        lax.fori_loop(0, own // together, some, 0)

    def start_state(slot):
        zero = jnp.zeros((ROWS, TILE), jnp.float32)
        row = jnp.zeros((1, TILE), jnp.float32)
        return tuple(zero for _ in range(lams_of(slot))) + (row, row)

    def tiles(slot, phase, first, last, state):
        lams = lambda_list(slot)
        softs = [2.0 - lam for lam in lams]
        count = fields_of(slot)
        unroll = max(u for u in (1, 2, UNROLL) if (last - first) % u == 0)

        def pair_sum(pair, state):
            word = order[slot, pair]
            same = (word & 1).astype(jnp.float32)
            mine = jnp.clip((word >> 1) & (2**row_bits - 1), 0, own - 1) * (count * PIECES)
            index = jnp.clip((word >> (1 + row_bits)) & (2**index_bits - 1), 0, near * span - 1)
            step_of = word >> (1 + row_bits + index_bits)
            col = [bufs[slot][0][index, f] for f in range(FIELDS)]
            if phase > 0:
                far = jnp.clip(jnp.where(step_of < near, 0, index), 0, span - 1)
                for part in range(1, phase + 1):
                    here = step_of == near + part - 1
                    col = [
                        jnp.where(here, bufs[slot][part][far, f], col[f]) for f in range(FIELDS)
                    ]
            fields = [jnp.broadcast_to(col[f], (ROWS, TILE)) for f in range(3)]
            charge_col = col[3]
            depth_col = col[4]
            size_col = jnp.broadcast_to(1.0 / col[5], (ROWS, TILE))
            sum_disp = [None] * len(lams)
            sum_coul = [None] * len(lams)
            for piece in range(PIECES):
                wide = [rowbs[slot][mine + (f * PIECES + piece)] for f in range(count)]
                dx = wide[0] - fields[0]
                dy = wide[1] - fields[1]
                dz = wide[2] - fields[2]
                r2 = dx * dx + dy * dy + dz * dz
                scaled = r2 * (wide[5] * size_col)
                cube = scaled * scaled * scaled
                for k in range(len(lams)):
                    inverse = 1.0 / (cube + wide[FIELDS + k])
                    disp = inverse * (inverse - wide[4])
                    coul = wide[3] * lax.rsqrt(r2 + softs[k])
                    if piece == 0:
                        sum_disp[k], sum_coul[k] = disp, coul
                    else:
                        sum_disp[k] = sum_disp[k] + disp
                        sum_coul[k] = sum_coul[k] + coul
            depth_four = 4.0 * depth_col
            totals = [
                state[k] + (sum_disp[k] * depth_four + sum_coul[k] * charge_col)
                for k in range(len(lams))
            ]
            return tuple(totals) + (
                state[-2] + same * (depth_col * depth_col),
                state[-1] + same * (charge_col * charge_col),
            )

        def some(step, state):
            for part in range(unroll):
                state = pair_sum(first + step * unroll + part, state)
            return state

        return lax.fori_loop(0, (last - first) // unroll, some, state)

    def close(slot, state):
        sums = []
        for k, lam in enumerate(lambda_list(slot)):
            core = jnp.full((1, TILE), 1.0 - 0.5 * lam, jnp.float32)
            soft = jnp.full((1, TILE), 2.0 - lam, jnp.float32)
            inverse = 1.0 / core
            own_pairs = state[-2] * (4.0 * inverse * (inverse - 1.0)) + state[-1] * lax.rsqrt(soft)
            line = jnp.sum(state[k], axis=0, keepdims=True) - own_pairs
            sums.append(jnp.sum(line, axis=1, keepdims=True) * lam)
        if two_ends and slot == 1:
            sums = [sums[0], jnp.where(win == 0, sums[0], sums[1]), sums[1]]
        return sums

    for slot in range(run):
        open_sends(slot)
    for slot in range(run):
        sort_pairs(slot)
    ordered = pltpu.make_async_copy(words, order, order_sem)
    ordered.start()
    spread(0)
    if dim_z > 1:
        pass_column(0, 1)
    if run > 1:
        pass_plane(1, 0)
    for slot in range(1, run):
        spread(slot)

    shares = []
    lowers = []
    for wl in range(run):
        window = win * run + wl
        odd = (window + parity[0]) & 1
        lower = window - odd
        threshold = thresholds[0]
        for v in range(1, windows):
            threshold = jnp.where(lower == v, thresholds[v], threshold)
        drawn = ((threshold + parity[0]) & 1073741823) + 1
        share = jnp.full((ROWS, TILE), drawn, jnp.int32).astype(jnp.float32) * (1.0 / 1073741824.0)
        shares.append(-jnp.log(share))
        lowers.append(lower)

    if dim_z > 2:
        pass_column(0, 2)
    if run > 1 and dim_z > 1:
        pass_column(1, 1)
    for step in range(3, dim_z):
        pass_column(0, step)
    ordered.wait()
    ends = phases_of(dims, groups, listed)

    def complete(slot, phase):
        steps = range(near) if phase == 0 else [near + phase - 1]
        for step in steps:
            if slot == 0:
                pass_plane(slot, step)
            last_arrivals(slot, step)

    if run > 1:
        later = [functools.partial(pass_plane, 1, step) for step in range(1, min(2, dim_z))]
        for step in range(2, dim_z):
            later.append(functools.partial(pass_column, 1, step))
        for step in range(2, dim_z):
            later.append(functools.partial(pass_plane, 1, step))
    else:
        later = []
    partial = []
    for slot in range(run):
        state = start_state(slot)
        first = 0
        if slot > 1:
            pass_plane(slot, 0)
            for step in range(1, dim_z):
                pass_column(slot, step)
            for step in range(1, dim_z):
                pass_plane(slot, step)
        cuts = []
        for phase, end in enumerate(ends):
            if slot == 0 and (end - first) % 8 == 0:
                cuts.append((phase, first, first + (end - first) // 2))
                cuts.append((phase, first + (end - first) // 2, end))
            else:
                cuts.append((phase, first, end))
            first = end
        done = -1
        for number, (phase, first, last) in enumerate(cuts):
            if phase != done:
                complete(slot, phase)
                done = phase
                if slot == 0 and phase == len(ends) - 1:
                    for partner in partners:
                        pl.semaphore_signal(ready, inc=1, device_id=partner, device_id_type=MESH)
            if last > first:
                state = tiles(slot, phase, first, last, state)
            if slot == 0 and later:
                later.pop(0)()
                if number == len(cuts) - 1:
                    while later:
                        later.pop(0)()
        partial.append(close(slot, state))

    lane = lax.broadcasted_iota(jnp.int32, (1, TILE), 1)
    line = jnp.zeros((1, TILE), jnp.float32)
    for slot in range(run):
        place = (win * run + window_of(slot)) * 3
        for k in range(3):
            line = jnp.where(lane == place + k, partial[slot][k], line)
    red[me] = line
    for _ in partners:
        pl.semaphore_wait(ready, 1)
    everyone = wins * groups
    for other_win in range(wins):
        for step in range(groups):
            if other_win or step:
                target = ((win + other_win) % wins, (grp + step) % groups)
                pltpu.make_async_remote_copy(
                    src_ref=red.at[me],
                    dst_ref=red.at[me],
                    send_sem=red_send.at[0],
                    recv_sem=red_recv.at[0],
                    device_id=target,
                    device_id_type=MESH,
                ).start()
    for copy in sent:
        copy.wait_send()
    rest = pltpu.make_async_remote_copy(
        src_ref=red.at[pl.ds(0, everyone - 1)],
        dst_ref=red.at[pl.ds(0, everyone - 1)],
        send_sem=red_send.at[0],
        recv_sem=red_recv.at[0],
        device_id=((win + 1) % wins, (grp + 1) % groups),
        device_id_type=MESH,
    )
    rest.wait_recv()
    rest.wait_send()
    scale = 1.0 / (listed * groups * TILE * TILE)
    total = jnp.sum(red[0:everyone], axis=0) * scale
    energy = [
        [jnp.sum(jnp.where(lane == v * 3 + k, total, 0.0)) for k in range(3)]
        for v in range(windows)
    ]
    ups = [e[2] - e[1] for e in energy]
    downs = [e[0] - e[1] for e in energy]
    rows = lax.broadcasted_iota(jnp.int32, (ROWS, TILE), 0)
    lanes = lax.broadcasted_iota(jnp.int32, (ROWS, TILE), 1)
    cell = rows * TILE + lanes
    result = jnp.zeros((ROWS, TILE), jnp.float32)
    for wl in range(run):
        window = win * run + wl
        for k in range(3):
            value = energy[wl][k]
            for part in range(1, wins):
                value = jnp.where(win == part, energy[part * run + wl][k], value)
            result = jnp.where(cell == wl * TILE + k, value, result)
        profile = jnp.float32(0.0)
        change = jnp.float32(0.0)
        for v in range(windows):
            profile = profile + jnp.where(v < window, ups[v], 0.0)
            change = change + jnp.where(lowers[wl] == v, ups[v], 0.0)
            change = change + jnp.where(lowers[wl] + 1 == v, downs[v], 0.0)
        result = jnp.where(cell == (run + 1) * TILE + wl, profile, result)
        partner = jnp.logical_and(lowers[wl] >= 0, lowers[wl] + 1 < windows)
        margin = shares[wl] - inverse_temp[0] * change
        margin = jnp.where(partner, margin, 0.0)
        result = jnp.where(cell == run * TILE + wl, margin, result)
    out[...] = result


def finish(run, total, out_energy, out_margin, out_profile):
    out_energy[...] = total[0:run, 0:3]
    out_margin[...] = total[run, 0:run]
    out_profile[...] = total[run + 1, 0:run]


def per_device(dims, atom_table, row_blocks, col_blocks, lambdas, inverse_temp, parity, thresholds):
    run, fields, atoms = atom_table.shape
    wins = lax.axis_size("win")
    groups = lax.axis_size("grp")
    own = atoms // TILE
    listed = row_blocks.shape[1]
    cfg = (run, wins, groups, own, listed, dims)
    hbm = pl.BlockSpec(memory_space=pltpu.HBM)
    vmem = pl.BlockSpec(memory_space=pltpu.VMEM)
    smem = pl.BlockSpec(memory_space=pltpu.SMEM)
    own_pad = -(-own // 8) * 8
    counts = [9] * run
    if wins == 2 and run == 2:
        counts[1] = 8
    near = near_steps(dims)
    span = dims[1] * dims[2] * own
    scratch = []
    for _ in range(run):
        for planes in [near] + [1] * (dims[0] - near):
            scratch.append(pltpu.VMEM((planes * span, FIELDS, 1, TILE), jnp.float32))
    scratch += [pltpu.VMEM((own * count * PIECES, ROWS, TILE), jnp.float32) for count in counts]
    scratch += [
        pltpu.VMEM((run, FIELDS, own_pad, TILE), jnp.float32),
        pltpu.VMEM((LINES * (own_pad + 1), TILE), jnp.float32),
        pltpu.VMEM((wins * groups, 1, TILE), jnp.float32),
        pltpu.VMEM((run, listed), jnp.int32),
        pltpu.VMEM((run, listed), jnp.int32),
        pltpu.VMEM((run, listed), jnp.int32),
        pltpu.SMEM((run, listed), jnp.int32),
        pltpu.SMEM((wins * run,), jnp.float32),
        pltpu.SMEM((wins * run,), jnp.int32),
        pltpu.SemaphoreType.DMA((2 * run,)),
        pltpu.SemaphoreType.DMA((4,)),
        pltpu.SemaphoreType.DMA((run, max(1, messages_of(dims)))),
        pltpu.SemaphoreType.DMA((run, dims[0], dims[1] * dims[2])),
        pltpu.SemaphoreType.DMA((1,)),
        pltpu.SemaphoreType.DMA((1,)),
        pltpu.SemaphoreType.REGULAR,
        pltpu.SemaphoreType.DMA,
    ]
    table = jnp.transpose(atom_table.reshape(run, fields, own, TILE), (1, 2, 0, 3))
    total = pl.pallas_call(
        functools.partial(kernel, cfg),
        out_shape=jax.ShapeDtypeStruct((8, TILE), jnp.float32),
        in_specs=[hbm, hbm, hbm, hbm, smem, smem, hbm],
        out_specs=vmem,
        scratch_shapes=scratch,
        compiler_params=pltpu.CompilerParams(
            collective_id=0, has_side_effects=True, vmem_limit_bytes=LIMIT
        ),
    )(table, row_blocks, col_blocks, lambdas, inverse_temp, parity, thresholds)
    shapes = (
        jax.ShapeDtypeStruct((run, 3), jnp.float32),
        jax.ShapeDtypeStruct((run,), jnp.float32),
        jax.ShapeDtypeStruct((run,), jnp.float32),
    )
    return pl.pallas_call(
        functools.partial(finish, run),
        out_shape=shapes,
        in_specs=[vmem],
        out_specs=(vmem, vmem, vmem),
        compiler_params=pltpu.CompilerParams(vmem_limit_bytes=1024 * 1024),
    )(total)


def solution(mesh):
    return jax.shard_map(
        functools.partial(per_device, grid_of(mesh)),
        mesh=mesh,
        in_specs=(P("win", None, "grp"), P("win", "grp"), P("win", "grp"), P(), P(), P(), P()),
        out_specs=(P("win", None), P("win"), P("win")),
        check_vma=False,
    )
```

```python
import functools

import jax
import jax.numpy as jnp
from jax import lax
from jax.experimental import pallas as pl
from jax.experimental.pallas import tpu as pltpu
from jax.sharding import PartitionSpec as P

TILE = 128
ROWS = 8
FIELDS = 6
PIECES = TILE // ROWS
UNROLL = 4
SPREAD = 4
LINES = 40
LIMIT = 67043328
MESH = pl.DeviceIdType.MESH


def grid_of(mesh):
    groups = mesh.shape["grp"]
    try:
        line = mesh.devices[0]
        coords = [tuple(d.coords) for d in line]
        dims = [len({c[a] for c in coords}) for a in (2, 1, 0)]
        base = [min(c[a] for c in coords) for a in (2, 1, 0)]
        want = [
            (base[2] + x, base[1] + y, base[0] + z)
            for z in range(dims[0])
            for y in range(dims[1])
            for x in range(dims[2])
        ]
        if [c[:3] for c in coords] == want:
            return tuple(dims)
    except Exception:
        pass
    return (groups, 1, 1)


def messages_of(dims):
    z, y, x = dims
    return (z - 1) + z * (x * y - 1)


def near_steps(dims):
    return min(2, dims[0])


def slots_of(groups, listed):
    return listed // groups + 1


def phases_of(dims, groups, listed):
    z, y, x = dims
    slots = slots_of(groups, listed)
    ends = []
    for step in range(near_steps(dims), z + 1):
        ends.append(max(0, listed - slots * (z - step) * y * x))
    return ends


def bits_for(count):
    return max(1, (count - 1).bit_length())


def split3(value):
    high = value.astype(jnp.bfloat16).astype(jnp.float32)
    rest = value - high
    middle = rest.astype(jnp.bfloat16).astype(jnp.float32)
    return high, middle, rest - middle


def kernel(
    cfg,
    table,
    row_hbm,
    col_hbm,
    lambdas_hbm,
    inverse_temp,
    parity,
    thresholds_hbm,
    out,
    *scratch,
):
    run, wins, groups, own, listed, dims = cfg
    dim_z, dim_y, dim_x = dims
    near = near_steps(dims)
    parts = dim_z - near + 1
    bufs = [scratch[slot * parts : (slot + 1) * parts] for slot in range(run)]
    scratch = scratch[run * parts :]
    zin = [scratch[slot * dim_z : (slot + 1) * dim_z] for slot in range(run)]
    scratch = scratch[run * dim_z :]
    rowbs = scratch[:run]
    (
        stage,
        feats,
        red,
        row_ids,
        col_ids,
        words,
        order,
        packs,
        asks,
        asked,
        lambdas,
        thresholds,
        load_sem,
        small_sem,
        send_sem,
        recv_sem,
        red_send,
        red_recv,
        ready,
        order_sem,
        ask_send,
        ask_recv,
        asked_sem,
    ) = scratch[run:]
    windows = wins * run
    win = lax.axis_index("win")
    grp = lax.axis_index("grp")
    my_z = grp // (dim_y * dim_x)
    my_y = (grp // dim_x) % dim_y
    my_x = grp % dim_x
    two_ends = wins == 2 and run == 2
    own_pad = stage.shape[2]
    me = win * groups + grp

    def window_of(slot):
        if two_ends:
            return jnp.where(win == 0, 1 - slot, slot)
        return slot

    def lams_of(slot):
        return 2 if two_ends and slot == 1 else 3

    def fields_of(slot):
        return FIELDS + lams_of(slot)

    plane = dim_y * dim_x
    span = plane * own
    row_bits = bits_for(own)
    slots = slots_of(groups, listed)
    unit = plane * slots
    index_bits = bits_for(near * unit)
    width = asks.shape[3]

    def group_at(z, dy, dx):
        return (z * dim_y + (my_y + dy) % dim_y) * dim_x + (my_x + dx) % dim_x

    def place_at(dy, dx):
        return ((my_y + dy) % dim_y) * dim_x + (my_x + dx) % dim_x

    paired = dim_z & (dim_z - 1) == 0

    def flipped(step):
        other = 0
        for bit in range(bits_for(dim_z)):
            mine = (my_z // 2**bit) % 2
            other = other + 2**bit * ((1 - mine) if (step >> bit) & 1 else mine)
        return other

    def plane_to(step):
        return flipped(step) if paired else (my_z + step) % dim_z

    def plane_from(step):
        return flipped(step) if paired else (my_z - step + dim_z) % dim_z

    def part_of(slot, step):
        if step < near:
            return bufs[slot][0], step * unit
        return bufs[slot][step - near + 1], 0

    def slots_at(slot, step, place):
        ref, base = part_of(slot, step)
        return ref.at[pl.ds(base + place * slots, slots)]

    my_place = place_at(0, 0)
    others = [(dy, dx) for dy in range(dim_y) for dx in range(dim_x) if dy or dx]

    loads = []
    for slot in range(run):
        local = window_of(slot)
        for f in range(FIELDS):
            loads.append(
                pltpu.make_async_copy(
                    table.at[f, :, local, :],
                    zin[slot][0].at[:, f, 0, :],
                    load_sem.at[slot],
                )
            )
    for slot in range(run):
        local = window_of(slot)
        loads.append(
            pltpu.make_async_copy(
                table.at[:, :, local, :],
                stage.at[slot, :, pl.ds(0, own), :],
                load_sem.at[run + slot],
            )
        )
    smalls = [
        pltpu.make_async_copy(row_hbm, row_ids, small_sem.at[0]),
        pltpu.make_async_copy(col_hbm, col_ids, small_sem.at[1]),
        pltpu.make_async_copy(lambdas_hbm, lambdas, small_sem.at[2]),
        pltpu.make_async_copy(thresholds_hbm, thresholds, small_sem.at[3]),
    ]
    for copy in loads:
        copy.start()
    for copy in smalls:
        copy.start()

    barrier = pltpu.get_barrier_semaphore()
    partners = [((win + step) % wins, grp) for step in range(1, wins)]
    peers = [(win, group_at(plane_to(step), 0, 0)) for step in range(1, dim_z)]
    peers += [(win, group_at(my_z, dy, dx)) for dy, dx in others]
    peers += partners
    for peer in peers:
        pl.semaphore_signal(barrier, inc=1, device_id=peer, device_id_type=MESH)

    for copy in smalls:
        copy.wait()

    def lambda_list(slot):
        window = win * run + window_of(slot)
        if two_ends and slot == 1:
            low = jnp.where(window == 0, 0, window - 1)
            return [lambdas[low], lambdas[low + 1]]
        return [
            lambdas[jnp.maximum(window - 1, 0)],
            lambdas[window],
            lambdas[jnp.minimum(window + 1, windows - 1)],
        ]

    def sort_pairs(slot):
        local = window_of(slot)
        rows = row_ids[pl.ds(local, 1), :]
        cols = col_ids[pl.ds(local, 1), :]
        zone = jnp.zeros((1, listed), jnp.int32)
        for z in range(1, dim_z):
            zone = zone + jnp.where(cols >= z * span, 1, 0)
        step_of = jnp.zeros((1, listed), jnp.int32)
        for step in range(1, dim_z):
            step_of = jnp.where(zone == plane_from(step), step, step_of)
        inside = cols - zone * span
        place = jnp.zeros((1, listed), jnp.int32)
        for spot in range(1, plane):
            place = place + jnp.where(inside >= spot * own, 1, 0)
        mine = jnp.clip(rows - grp * own, 0, own - 1)
        key = place * dim_z + step_of
        packed = (key * 2**row_bits + (inside - place * own)) * 2**row_bits + mine
        packed = packed * 2 + jnp.where(rows == cols, 1, 0)
        lane = lax.broadcasted_iota(jnp.int32, (listed, listed), 1)
        line = lax.broadcasted_iota(jnp.int32, (listed, listed), 0)
        packed_row = jnp.broadcast_to(packed.astype(jnp.float32), (listed, listed))
        packed_col = jnp.sum(jnp.where(lane == line, packed_row, 0.0), axis=1, keepdims=True)
        packed_col = jnp.broadcast_to(packed_col.astype(jnp.int32), (listed, listed))
        low = packed_col & (2 ** (row_bits + 1) - 1)
        block = (packed_col >> (row_bits + 1)) & (2**row_bits - 1)
        key_col = packed_col >> (2 * row_bits + 1)
        key_row = jnp.broadcast_to(key, (listed, listed))
        earlier = jnp.where(jnp.logical_and(key_row == key_col, lane < line), 1.0, 0.0)
        count = jnp.sum(earlier, axis=1, keepdims=True).astype(jnp.int32)
        count = jnp.minimum(jnp.broadcast_to(count, (listed, listed)), slots - 1)
        step_col = key_col % dim_z
        place_col = key_col // dim_z
        rank_col = step_col * listed + line
        rank_row = jnp.broadcast_to(step_of, (listed, listed)) * listed + lane
        before = jnp.where(rank_row < rank_col, 1.0, 0.0)
        target = jnp.sum(before, axis=1, keepdims=True).astype(jnp.int32)
        index = place_col * slots + count
        index = index + jnp.where(step_col < near, step_col, 0) * unit
        word = (step_col * 2**index_bits + index) * 2 ** (row_bits + 1) + low
        hit = jnp.broadcast_to(target, (listed, listed)) == lane
        sorted_row = jnp.sum(jnp.where(hit, word.astype(jnp.float32), 0.0), axis=0, keepdims=True)
        words[pl.ds(slot, 1), :] = sorted_row.astype(jnp.int32)
        wide_lane = lax.broadcasted_iota(jnp.int32, (listed, width), 1)
        spots = (key_col * slots + count)[:, 0:1]
        chosen = jnp.where(
            jnp.broadcast_to(spots, (listed, width)) == wide_lane,
            jnp.broadcast_to(block[:, 0:1], (listed, width)).astype(jnp.float32),
            0.0,
        )
        asks[my_place, slot] = jnp.sum(chosen, axis=0, keepdims=True).astype(jnp.int32)

    for slot in range(run):
        sort_pairs(slot)

    for copy in loads:
        copy.wait()

    pl.semaphore_wait(barrier, len(peers))

    counts = [0] * run
    sent = []

    def begin(source, target, number, receive, peer, slot):
        copy = pltpu.make_async_remote_copy(
            src_ref=source,
            dst_ref=target,
            send_sem=send_sem.at[slot, number],
            recv_sem=receive,
            device_id={"grp": peer},
            device_id_type=MESH,
        )
        return copy

    def send(slot, source, target, receive, peer):
        copy = begin(source, target, counts[slot], receive, peer, slot)
        counts[slot] += 1
        copy.start()
        sent.append(copy)

    asking = []
    for number, (dy, dx) in enumerate(others):
        asking.append(
            pltpu.make_async_remote_copy(
                src_ref=asks.at[my_place],
                dst_ref=asks.at[my_place],
                send_sem=ask_send.at[number],
                recv_sem=ask_recv.at[my_place],
                device_id={"grp": group_at(my_z, dy, dx)},
                device_id_type=MESH,
            )
        )
    for copy in asking:
        copy.start()

    def questions():
        for dy, dx in others:
            place = place_at(dy, dx)
            pltpu.make_async_remote_copy(
                src_ref=asks.at[place],
                dst_ref=asks.at[place],
                send_sem=ask_send.at[0],
                recv_sem=ask_recv.at[place],
                device_id={"grp": group_at(my_z, dy, dx)},
                device_id_type=MESH,
            ).wait_recv()
        copy = pltpu.make_async_copy(asks, asked, asked_sem)
        copy.start()
        return copy

    def open_sends(slot):
        for step in range(1, dim_z):
            peer = group_at(plane_to(step), 0, 0)
            send(slot, zin[slot][0], zin[slot][step], recv_sem.at[slot, step, my_place], peer)

    def answer(slot, step):
        if step:
            share = zin[slot][step]
            begin(share, share, 0, recv_sem.at[slot, step, my_place], grp, slot).wait_recv()
        share = zin[slot][step]

        def named(place, part):
            block = asked[place, slot, 0, (my_place * dim_z + step) * slots + part]
            return jnp.clip(block, 0, own - 1)

        for number, (dy, dx) in enumerate(others):
            first = (step * len(others) + number) * slots
            for part in range(slots):
                block = named(place_at(dy, dx), part)
                for f in range(FIELDS):
                    packs[slot, first + part, f] = share[block, f]
        for number, (dy, dx) in enumerate(others):
            first = (step * len(others) + number) * slots
            send(
                slot,
                packs.at[slot, pl.ds(first, slots)],
                slots_at(slot, step, my_place),
                recv_sem.at[slot, step, my_place],
                group_at(my_z, dy, dx),
            )
        ref, base = part_of(slot, step)
        for part in range(slots):
            block = named(my_place, part)
            for f in range(FIELDS):
                ref[base + my_place * slots + part, f] = share[block, f]

    def answered(slot, step):
        for dy, dx in others:
            place = place_at(dy, dx)
            ref = slots_at(slot, step, place)
            begin(ref, ref, 0, recv_sem.at[slot, step, place], grp, slot).wait_recv()

    def spread(slot):
        lams = lambda_list(slot)
        count = fields_of(slot)
        depth = stage[slot, 4]
        inverse_root = lax.rsqrt(depth)
        sixth = jnp.exp(jnp.log(depth) * (-1.0 / 6.0))
        values = [stage[slot, f] for f in range(4)]
        values += [depth * inverse_root, sixth / stage[slot, 5]]
        values += [inverse_root * (1.0 - 0.5 * lam) for lam in lams]
        for f, value in enumerate(values):
            for part, piece in enumerate(split3(value)):
                feats[pl.ds(part * count + f, own_pad, stride=LINES), :] = piece
        for row in range(3 * count, 32):
            feats[pl.ds(row, own_pad, stride=LINES), :] = jnp.zeros((own_pad, TILE), jnp.float32)
        source = lax.broadcasted_iota(jnp.int32, (32, count * TILE), 0)
        target = lax.broadcasted_iota(jnp.int32, (32, count * TILE), 1) // TILE
        picks = jnp.zeros((32, count * TILE), jnp.float32)
        for part in range(3):
            picks = jnp.where(source == target + part * count, 1.0, picks)
        picks = picks.astype(jnp.bfloat16)

        def one(block):
            start = pl.multiple_of(block * LINES, 8)
            lines = feats[pl.ds(start, 32), :].astype(jnp.bfloat16)
            wide = lax.dot_general(
                lines, picks, (((0,), (0,)), ((), ())), preferred_element_type=jnp.float32
            )
            for f in range(count):
                for piece in range(PIECES):
                    rowbs[slot][(block * count + f) * PIECES + piece] = wide[
                        piece * ROWS : (piece + 1) * ROWS, f * TILE : (f + 1) * TILE
                    ]

        def some(step, carry):
            for part in range(together):
                one(step * together + part)
            return carry

        together = SPREAD if own % SPREAD == 0 else 1
        lax.fori_loop(0, own // together, some, 0)

    def start_state(slot):
        zero = jnp.zeros((ROWS, TILE), jnp.float32)
        row = jnp.zeros((1, TILE), jnp.float32)
        return tuple(zero for _ in range(lams_of(slot))) + (row, row)

    def tiles(slot, phase, first, last, state):
        lams = lambda_list(slot)
        softs = [2.0 - lam for lam in lams]
        count = fields_of(slot)
        unroll = max(u for u in (1, 2, UNROLL) if (last - first) % u == 0)

        def pair_sum(pair, state):
            word = order[slot, pair]
            same = (word & 1).astype(jnp.float32)
            mine = jnp.clip((word >> 1) & (2**row_bits - 1), 0, own - 1) * (count * PIECES)
            index = jnp.clip((word >> (1 + row_bits)) & (2**index_bits - 1), 0, near * unit - 1)
            step_of = word >> (1 + row_bits + index_bits)
            col = [bufs[slot][0][index, f] for f in range(FIELDS)]
            if phase > 0:
                far = jnp.clip(jnp.where(step_of < near, 0, index), 0, unit - 1)
                for part in range(1, phase + 1):
                    here = step_of == near + part - 1
                    col = [
                        jnp.where(here, bufs[slot][part][far, f], col[f]) for f in range(FIELDS)
                    ]
            fields = [jnp.broadcast_to(col[f], (ROWS, TILE)) for f in range(3)]
            charge_col = col[3]
            depth_col = col[4]
            size_col = jnp.broadcast_to(1.0 / col[5], (ROWS, TILE))
            sum_disp = [None] * len(lams)
            sum_coul = [None] * len(lams)
            for piece in range(PIECES):
                wide = [rowbs[slot][mine + (f * PIECES + piece)] for f in range(count)]
                dx = wide[0] - fields[0]
                dy = wide[1] - fields[1]
                dz = wide[2] - fields[2]
                r2 = dx * dx + dy * dy + dz * dz
                scaled = r2 * (wide[5] * size_col)
                cube = scaled * scaled * scaled
                for k in range(len(lams)):
                    inverse = 1.0 / (cube + wide[FIELDS + k])
                    disp = inverse * (inverse - wide[4])
                    coul = wide[3] * lax.rsqrt(r2 + softs[k])
                    if piece == 0:
                        sum_disp[k], sum_coul[k] = disp, coul
                    else:
                        sum_disp[k] = sum_disp[k] + disp
                        sum_coul[k] = sum_coul[k] + coul
            depth_four = 4.0 * depth_col
            totals = [
                state[k] + (sum_disp[k] * depth_four + sum_coul[k] * charge_col)
                for k in range(len(lams))
            ]
            return tuple(totals) + (
                state[-2] + same * (depth_col * depth_col),
                state[-1] + same * (charge_col * charge_col),
            )

        def some(step, state):
            for part in range(unroll):
                state = pair_sum(first + step * unroll + part, state)
            return state

        return lax.fori_loop(0, (last - first) // unroll, some, state)

    def close(slot, state):
        sums = []
        for k, lam in enumerate(lambda_list(slot)):
            core = jnp.full((1, TILE), 1.0 - 0.5 * lam, jnp.float32)
            soft = jnp.full((1, TILE), 2.0 - lam, jnp.float32)
            inverse = 1.0 / core
            own_pairs = state[-2] * (4.0 * inverse * (inverse - 1.0)) + state[-1] * lax.rsqrt(soft)
            line = jnp.sum(state[k], axis=0, keepdims=True) - own_pairs
            sums.append(jnp.sum(line, axis=1, keepdims=True) * lam)
        if two_ends and slot == 1:
            sums = [sums[0], jnp.where(win == 0, sums[0], sums[1]), sums[1]]
        return sums

    for slot in range(run):
        open_sends(slot)
    ordered = pltpu.make_async_copy(words, order, order_sem)
    ordered.start()
    spread(0)
    known = questions()
    known.wait()
    answer(0, 0)
    if dim_z > 1:
        answer(0, 1)
    for slot in range(1, run):
        answer(slot, 0)
    for slot in range(1, run):
        spread(slot)

    shares = []
    lowers = []
    for wl in range(run):
        window = win * run + wl
        odd = (window + parity[0]) & 1
        lower = window - odd
        threshold = thresholds[0]
        for v in range(1, windows):
            threshold = jnp.where(lower == v, thresholds[v], threshold)
        drawn = ((threshold + parity[0]) & 1073741823) + 1
        share = jnp.full((ROWS, TILE), drawn, jnp.int32).astype(jnp.float32) * (1.0 / 1073741824.0)
        shares.append(-jnp.log(share))
        lowers.append(lower)

    for step in range(2, dim_z):
        answer(0, step)
        if run > 1:
            answer(1, step - 1)
    ordered.wait()
    ends = phases_of(dims, groups, listed)

    def complete(slot, phase):
        for step in range(near) if phase == 0 else [near + phase - 1]:
            answered(slot, step)

    later = []
    for slot in range(1, run):
        first_step = dim_z - 1 if slot == 1 and dim_z > 2 else 1
        later += [functools.partial(answer, slot, step) for step in range(first_step, dim_z)]
    partial = []
    for slot in range(run):
        state = start_state(slot)
        first = 0
        for phase, end in enumerate(ends):
            complete(slot, phase)
            if slot == 0 and phase == len(ends) - 1:
                for partner in partners:
                    pl.semaphore_signal(ready, inc=1, device_id=partner, device_id_type=MESH)
            if end > first:
                state = tiles(slot, phase, first, end, state)
            first = end
            if slot == 0 and later:
                later.pop(0)()
        while later:
            later.pop(0)()
        partial.append(close(slot, state))

    lane = lax.broadcasted_iota(jnp.int32, (1, TILE), 1)
    line = jnp.zeros((1, TILE), jnp.float32)
    for slot in range(run):
        place = (win * run + window_of(slot)) * 3
        for k in range(3):
            line = jnp.where(lane == place + k, partial[slot][k], line)
    red[me] = line
    for _ in partners:
        pl.semaphore_wait(ready, 1)
    everyone = wins * groups
    for other_win in range(wins):
        for step in range(groups):
            if other_win or step:
                target = ((win + other_win) % wins, (grp + step) % groups)
                pltpu.make_async_remote_copy(
                    src_ref=red.at[me],
                    dst_ref=red.at[me],
                    send_sem=red_send.at[0],
                    recv_sem=red_recv.at[0],
                    device_id=target,
                    device_id_type=MESH,
                ).start()
    for copy in sent + asking:
        copy.wait_send()
    rest = pltpu.make_async_remote_copy(
        src_ref=red.at[pl.ds(0, everyone - 1)],
        dst_ref=red.at[pl.ds(0, everyone - 1)],
        send_sem=red_send.at[0],
        recv_sem=red_recv.at[0],
        device_id=((win + 1) % wins, (grp + 1) % groups),
        device_id_type=MESH,
    )
    rest.wait_recv()
    rest.wait_send()
    scale = 1.0 / (listed * groups * TILE * TILE)
    total = jnp.sum(red[0:everyone], axis=0) * scale
    energy = [
        [jnp.sum(jnp.where(lane == v * 3 + k, total, 0.0)) for k in range(3)]
        for v in range(windows)
    ]
    ups = [e[2] - e[1] for e in energy]
    downs = [e[0] - e[1] for e in energy]
    rows = lax.broadcasted_iota(jnp.int32, (ROWS, TILE), 0)
    lanes = lax.broadcasted_iota(jnp.int32, (ROWS, TILE), 1)
    cell = rows * TILE + lanes
    result = jnp.zeros((ROWS, TILE), jnp.float32)
    for wl in range(run):
        window = win * run + wl
        for k in range(3):
            value = energy[wl][k]
            for part in range(1, wins):
                value = jnp.where(win == part, energy[part * run + wl][k], value)
            result = jnp.where(cell == wl * TILE + k, value, result)
        profile = jnp.float32(0.0)
        change = jnp.float32(0.0)
        for v in range(windows):
            profile = profile + jnp.where(v < window, ups[v], 0.0)
            change = change + jnp.where(lowers[wl] == v, ups[v], 0.0)
            change = change + jnp.where(lowers[wl] + 1 == v, downs[v], 0.0)
        result = jnp.where(cell == (run + 1) * TILE + wl, profile, result)
        partner = jnp.logical_and(lowers[wl] >= 0, lowers[wl] + 1 < windows)
        margin = shares[wl] - inverse_temp[0] * change
        margin = jnp.where(partner, margin, 0.0)
        result = jnp.where(cell == run * TILE + wl, margin, result)
    out[...] = result


def finish(run, total, out_energy, out_margin, out_profile):
    out_energy[...] = total[0:run, 0:3]
    out_margin[...] = total[run, 0:run]
    out_profile[...] = total[run + 1, 0:run]


def per_device(dims, atom_table, row_blocks, col_blocks, lambdas, inverse_temp, parity, thresholds):
    run, fields, atoms = atom_table.shape
    wins = lax.axis_size("win")
    groups = lax.axis_size("grp")
    own = atoms // TILE
    listed = row_blocks.shape[1]
    cfg = (run, wins, groups, own, listed, dims)
    hbm = pl.BlockSpec(memory_space=pltpu.HBM)
    vmem = pl.BlockSpec(memory_space=pltpu.VMEM)
    smem = pl.BlockSpec(memory_space=pltpu.SMEM)
    own_pad = -(-own // 8) * 8
    counts = [9] * run
    if wins == 2 and run == 2:
        counts[1] = 8
    near = near_steps(dims)
    plane = dims[1] * dims[2]
    slots = slots_of(groups, listed)
    unit = plane * slots
    width = -(-plane * dims[0] * slots // TILE) * TILE
    answers = max(1, dims[0] * (plane - 1) * slots)
    scratch = []
    for _ in range(run):
        for planes in [near] + [1] * (dims[0] - near):
            scratch.append(pltpu.VMEM((planes * unit, FIELDS, 1, TILE), jnp.float32))
    scratch += [pltpu.VMEM((own, FIELDS, 1, TILE), jnp.float32) for _ in range(run * dims[0])]
    scratch += [pltpu.VMEM((own * count * PIECES, ROWS, TILE), jnp.float32) for count in counts]
    scratch += [
        pltpu.VMEM((run, FIELDS, own_pad, TILE), jnp.float32),
        pltpu.VMEM((LINES * (own_pad + 1), TILE), jnp.float32),
        pltpu.VMEM((wins * groups, 1, TILE), jnp.float32),
        pltpu.VMEM((run, listed), jnp.int32),
        pltpu.VMEM((run, listed), jnp.int32),
        pltpu.VMEM((run, listed), jnp.int32),
        pltpu.SMEM((run, listed), jnp.int32),
        pltpu.VMEM((run, answers, FIELDS, 1, TILE), jnp.float32),
        pltpu.VMEM((plane, run, 1, width), jnp.int32),
        pltpu.SMEM((plane, run, 1, width), jnp.int32),
        pltpu.SMEM((wins * run,), jnp.float32),
        pltpu.SMEM((wins * run,), jnp.int32),
        pltpu.SemaphoreType.DMA((2 * run,)),
        pltpu.SemaphoreType.DMA((4,)),
        pltpu.SemaphoreType.DMA((run, max(1, messages_of(dims)))),
        pltpu.SemaphoreType.DMA((run, dims[0], dims[1] * dims[2])),
        pltpu.SemaphoreType.DMA((1,)),
        pltpu.SemaphoreType.DMA((1,)),
        pltpu.SemaphoreType.REGULAR,
        pltpu.SemaphoreType.DMA,
        pltpu.SemaphoreType.DMA((plane,)),
        pltpu.SemaphoreType.DMA((plane,)),
        pltpu.SemaphoreType.DMA,
    ]
    table = jnp.transpose(atom_table.reshape(run, fields, own, TILE), (1, 2, 0, 3))
    total = pl.pallas_call(
        functools.partial(kernel, cfg),
        out_shape=jax.ShapeDtypeStruct((8, TILE), jnp.float32),
        in_specs=[hbm, hbm, hbm, hbm, smem, smem, hbm],
        out_specs=vmem,
        scratch_shapes=scratch,
        compiler_params=pltpu.CompilerParams(
            collective_id=0, has_side_effects=True, vmem_limit_bytes=LIMIT
        ),
    )(table, row_blocks, col_blocks, lambdas, inverse_temp, parity, thresholds)
    shapes = (
        jax.ShapeDtypeStruct((run, 3), jnp.float32),
        jax.ShapeDtypeStruct((run,), jnp.float32),
        jax.ShapeDtypeStruct((run,), jnp.float32),
    )
    return pl.pallas_call(
        functools.partial(finish, run),
        out_shape=shapes,
        in_specs=[vmem],
        out_specs=(vmem, vmem, vmem),
        compiler_params=pltpu.CompilerParams(vmem_limit_bytes=1024 * 1024),
    )(total)


def solution(mesh):
    return jax.shard_map(
        functools.partial(per_device, grid_of(mesh)),
        mesh=mesh,
        in_specs=(P("win", None, "grp"), P("win", "grp"), P("win", "grp"), P(), P(), P(), P()),
        out_specs=(P("win", None), P("win"), P("win")),
        check_vma=False,
    )
```

```python
import functools
import itertools

import jax
import jax.numpy as jnp
from jax import lax
from jax.experimental import pallas as pl
from jax.experimental.pallas import tpu as pltpu
from jax.sharding import PartitionSpec as P

TILE = 128
ROWS = 8
FIELDS = 6
PIECES = TILE // ROWS
UNROLL = 4
SPREAD = 4
HEAD = 3
LINES = 40
LIMIT = 67043328
MESH = pl.DeviceIdType.MESH


def grid_of(mesh):
    groups = mesh.shape["grp"]
    try:
        line = mesh.devices[0]
        coords = [tuple(d.coords) for d in line]
        dims = [len({c[a] for c in coords}) for a in (2, 1, 0)]
        base = [min(c[a] for c in coords) for a in (2, 1, 0)]
        want = [
            (base[2] + x, base[1] + y, base[0] + z)
            for z in range(dims[0])
            for y in range(dims[1])
            for x in range(dims[2])
        ]
        if [c[:3] for c in coords] == want:
            return tuple(dims)
    except Exception:
        pass
    return (groups, 1, 1)


def messages_of(dims):
    z, y, x = dims
    return (z - 1) + z * (x * y - 1)


def near_steps(dims):
    return min(2, dims[0])


def backward(count):
    return range(count - 1, -1, -1)


def slots_of(groups, listed):
    return listed // groups + 1


def phases_of(dims, groups, listed):
    z, y, x = dims
    slots = slots_of(groups, listed)
    ends = []
    for step in range(near_steps(dims), z + 1):
        ends.append(max(0, listed - slots * (z - step) * y * x))
    return ends


def bits_for(count):
    return max(1, (count - 1).bit_length())


def split3(value):
    high = value.astype(jnp.bfloat16).astype(jnp.float32)
    rest = value - high
    middle = rest.astype(jnp.bfloat16).astype(jnp.float32)
    return high, middle, rest - middle


def kernel(
    cfg,
    table,
    row_hbm,
    col_hbm,
    lambdas_hbm,
    inverse_temp,
    parity,
    thresholds_hbm,
    out,
    *scratch,
):
    run, wins, groups, own, listed, dims = cfg
    dim_z, dim_y, dim_x = dims
    near = near_steps(dims)
    parts = dim_z - near + 1
    bufs = [scratch[slot * parts : (slot + 1) * parts] for slot in range(run)]
    scratch = scratch[run * parts :]
    zin = [scratch[slot * dim_z : (slot + 1) * dim_z] for slot in range(run)]
    scratch = scratch[run * dim_z :]
    rowbs = scratch[:run]
    (
        stage,
        feats,
        red,
        row_ids,
        col_ids,
        words,
        order,
        packs,
        asks,
        asked,
        lambdas,
        thresholds,
        load_sem,
        small_sem,
        send_sem,
        recv_sem,
        red_send,
        red_recv,
        ready,
        order_sem,
        ask_send,
        ask_recv,
        asked_sem,
    ) = scratch[run:]
    windows = wins * run
    win = lax.axis_index("win")
    grp = lax.axis_index("grp")
    my_z = grp // (dim_y * dim_x)
    my_y = (grp // dim_x) % dim_y
    my_x = grp % dim_x
    two_ends = wins == 2 and run == 2
    own_pad = stage.shape[2]
    me = win * groups + grp

    def window_of(slot):
        if two_ends:
            return jnp.where(win == 0, 1 - slot, slot)
        return slot

    def lams_of(slot):
        return 2 if two_ends and slot == 1 else 3

    def fields_of(slot):
        return FIELDS + lams_of(slot)

    plane = dim_y * dim_x
    span = plane * own
    row_bits = bits_for(own)
    slots = slots_of(groups, listed)
    unit = plane * slots
    index_bits = bits_for(near * unit)
    width = asks.shape[3]

    def group_at(z, dy, dx):
        return (z * dim_y + (my_y + dy) % dim_y) * dim_x + (my_x + dx) % dim_x

    def place_at(dy, dx):
        return ((my_y + dy) % dim_y) * dim_x + (my_x + dx) % dim_x

    paired = dim_z & (dim_z - 1) == 0

    def flipped(step):
        other = 0
        for bit in range(bits_for(dim_z)):
            mine = (my_z // 2**bit) % 2
            other = other + 2**bit * ((1 - mine) if (step >> bit) & 1 else mine)
        return other

    def plane_to(step):
        return flipped(step) if paired else (my_z + step) % dim_z

    def plane_from(step):
        return flipped(step) if paired else (my_z - step + dim_z) % dim_z

    def part_of(slot, step):
        if step < near:
            return bufs[slot][0], step * unit
        return bufs[slot][step - near + 1], 0

    def slots_at(slot, step, place):
        ref, base = part_of(slot, step)
        return ref.at[pl.ds(base + place * slots, slots)]

    my_place = place_at(0, 0)
    others = [(dy, dx) for dy in range(dim_y) for dx in range(dim_x) if dy or dx]

    loads = []
    for slot in range(run):
        local = window_of(slot)
        for f in range(FIELDS):
            loads.append(
                pltpu.make_async_copy(
                    table.at[f, :, local, :],
                    zin[slot][0].at[:, f, 0, :],
                    load_sem.at[slot],
                )
            )
    for slot in range(run):
        local = window_of(slot)
        loads.append(
            pltpu.make_async_copy(
                table.at[:, :, local, :],
                stage.at[slot, :, pl.ds(0, own), :],
                load_sem.at[run + slot],
            )
        )
    smalls = [
        pltpu.make_async_copy(row_hbm, row_ids, small_sem.at[0]),
        pltpu.make_async_copy(col_hbm, col_ids, small_sem.at[1]),
        pltpu.make_async_copy(lambdas_hbm, lambdas, small_sem.at[2]),
        pltpu.make_async_copy(thresholds_hbm, thresholds, small_sem.at[3]),
    ]
    for copy in loads:
        copy.start()
    for copy in smalls:
        copy.start()

    barrier = pltpu.get_barrier_semaphore()
    partners = [((win + step) % wins, grp) for step in range(1, wins)]
    peers = [(win, group_at(plane_to(step), 0, 0)) for step in range(1, dim_z)]
    peers += [(win, group_at(my_z, dy, dx)) for dy, dx in others]
    peers += partners
    for peer in peers:
        pl.semaphore_signal(barrier, inc=1, device_id=peer, device_id_type=MESH)

    for copy in smalls:
        copy.wait()

    def lambda_list(slot):
        window = win * run + window_of(slot)
        if two_ends and slot == 1:
            low = jnp.where(window == 0, 0, window - 1)
            return [lambdas[low], lambdas[low + 1]]
        return [
            lambdas[jnp.maximum(window - 1, 0)],
            lambdas[window],
            lambdas[jnp.minimum(window + 1, windows - 1)],
        ]

    def sort_pairs(slot):
        local = window_of(slot)
        rows = row_ids[pl.ds(local, 1), :]
        cols = col_ids[pl.ds(local, 1), :]
        zone = jnp.zeros((1, listed), jnp.int32)
        for z in range(1, dim_z):
            zone = zone + jnp.where(cols >= z * span, 1, 0)
        step_of = jnp.zeros((1, listed), jnp.int32)
        for step in range(1, dim_z):
            step_of = jnp.where(zone == plane_from(step), step, step_of)
        inside = cols - zone * span
        place = jnp.zeros((1, listed), jnp.int32)
        for spot in range(1, plane):
            place = place + jnp.where(inside >= spot * own, 1, 0)
        mine = jnp.clip(rows - grp * own, 0, own - 1)
        key = place * dim_z + step_of
        packed = (key * 2**row_bits + (inside - place * own)) * 2**row_bits + mine
        packed = packed * 2 + jnp.where(rows == cols, 1, 0)
        lane = lax.broadcasted_iota(jnp.int32, (listed, listed), 1)
        line = lax.broadcasted_iota(jnp.int32, (listed, listed), 0)
        packed_row = jnp.broadcast_to(packed.astype(jnp.float32), (listed, listed))
        packed_col = jnp.sum(jnp.where(lane == line, packed_row, 0.0), axis=1, keepdims=True)
        packed_col = jnp.broadcast_to(packed_col.astype(jnp.int32), (listed, listed))
        low = packed_col & (2 ** (row_bits + 1) - 1)
        block = (packed_col >> (row_bits + 1)) & (2**row_bits - 1)
        key_col = packed_col >> (2 * row_bits + 1)
        key_row = jnp.broadcast_to(key, (listed, listed))
        earlier = jnp.where(jnp.logical_and(key_row == key_col, lane < line), 1.0, 0.0)
        count = jnp.sum(earlier, axis=1, keepdims=True).astype(jnp.int32)
        count = jnp.minimum(jnp.broadcast_to(count, (listed, listed)), slots - 1)
        step_col = key_col % dim_z
        place_col = key_col // dim_z
        rank_col = step_col * listed + line
        rank_row = jnp.broadcast_to(step_of, (listed, listed)) * listed + lane
        before = jnp.where(rank_row < rank_col, 1.0, 0.0)
        target = jnp.sum(before, axis=1, keepdims=True).astype(jnp.int32)
        index = place_col * slots + count
        index = index + jnp.where(step_col < near, step_col, 0) * unit
        word = (step_col * 2**index_bits + index) * 2 ** (row_bits + 1) + low
        hit = jnp.broadcast_to(target, (listed, listed)) == lane
        sorted_row = jnp.sum(jnp.where(hit, word.astype(jnp.float32), 0.0), axis=0, keepdims=True)
        words[pl.ds(slot, 1), :] = sorted_row.astype(jnp.int32)
        wide_lane = lax.broadcasted_iota(jnp.int32, (listed, width), 1)
        spots = (key_col * slots + count)[:, 0:1]
        chosen = jnp.where(
            jnp.broadcast_to(spots, (listed, width)) == wide_lane,
            jnp.broadcast_to(block[:, 0:1], (listed, width)).astype(jnp.float32),
            0.0,
        )
        asks[my_place, slot] = jnp.sum(chosen, axis=0, keepdims=True).astype(jnp.int32)

    for slot in range(run):
        sort_pairs(slot)

    for copy in loads:
        copy.wait()

    pl.semaphore_wait(barrier, len(peers))

    counts = [0] * run
    sent = []

    def begin(source, target, number, receive, peer, slot):
        copy = pltpu.make_async_remote_copy(
            src_ref=source,
            dst_ref=target,
            send_sem=send_sem.at[slot, number],
            recv_sem=receive,
            device_id={"grp": peer},
            device_id_type=MESH,
        )
        return copy

    def send(slot, source, target, receive, peer):
        copy = begin(source, target, counts[slot], receive, peer, slot)
        counts[slot] += 1
        copy.start()
        sent.append(copy)

    asking = []
    for number, (dy, dx) in enumerate(others):
        asking.append(
            pltpu.make_async_remote_copy(
                src_ref=asks.at[my_place],
                dst_ref=asks.at[my_place],
                send_sem=ask_send.at[number],
                recv_sem=ask_recv.at[my_place],
                device_id={"grp": group_at(my_z, dy, dx)},
                device_id_type=MESH,
            )
        )
    for copy in asking:
        copy.start()

    def questions():
        for dy, dx in others:
            place = place_at(dy, dx)
            pltpu.make_async_remote_copy(
                src_ref=asks.at[place],
                dst_ref=asks.at[place],
                send_sem=ask_send.at[0],
                recv_sem=ask_recv.at[place],
                device_id={"grp": group_at(my_z, dy, dx)},
                device_id_type=MESH,
            ).wait_recv()
        copy = pltpu.make_async_copy(asks, asked, asked_sem)
        copy.start()
        return copy

    def open_sends(slot):
        for step in range(1, dim_z):
            peer = group_at(plane_to(step), 0, 0)
            send(slot, zin[slot][0], zin[slot][step], recv_sem.at[slot, step, my_place], peer)

    def answer(slot, step):
        if step:
            share = zin[slot][step]
            begin(share, share, 0, recv_sem.at[slot, step, my_place], grp, slot).wait_recv()
        share = zin[slot][step]

        def named(place, part):
            block = asked[place, slot, 0, (my_place * dim_z + step) * slots + part]
            return jnp.clip(block, 0, own - 1)

        for number, (dy, dx) in enumerate(others):
            first = (step * len(others) + number) * slots
            for part in range(slots):
                block = named(place_at(dy, dx), part)
                for f in range(FIELDS):
                    packs[slot, first + part, f] = share[block, f]
        for number, (dy, dx) in enumerate(others):
            first = (step * len(others) + number) * slots
            send(
                slot,
                packs.at[slot, pl.ds(first, slots)],
                slots_at(slot, step, my_place),
                recv_sem.at[slot, step, my_place],
                group_at(my_z, dy, dx),
            )
        ref, base = part_of(slot, step)
        for part in range(slots):
            block = named(my_place, part)
            for f in range(FIELDS):
                ref[base + my_place * slots + part, f] = share[block, f]

    def answered(slot, step):
        for dy, dx in others:
            place = place_at(dy, dx)
            ref = slots_at(slot, step, place)
            begin(ref, ref, 0, recv_sem.at[slot, step, place], grp, slot).wait_recv()

    def spread(slot):
        lams = lambda_list(slot)
        count = fields_of(slot)
        depth = stage[slot, 4]
        inverse_root = lax.rsqrt(depth)
        sixth = jnp.exp(jnp.log(depth) * (-1.0 / 6.0))
        values = [stage[slot, f] for f in range(4)]
        values += [depth * inverse_root, sixth / stage[slot, 5]]
        values += [inverse_root * (1.0 - 0.5 * lam) for lam in lams]
        for f, value in enumerate(values):
            for part, piece in enumerate(split3(value)):
                feats[pl.ds(part * count + f, own_pad, stride=LINES), :] = piece
        for row in range(3 * count, 32):
            feats[pl.ds(row, own_pad, stride=LINES), :] = jnp.zeros((own_pad, TILE), jnp.float32)
        source = lax.broadcasted_iota(jnp.int32, (32, count * TILE), 0)
        target = lax.broadcasted_iota(jnp.int32, (32, count * TILE), 1) // TILE
        picks = jnp.zeros((32, count * TILE), jnp.float32)
        for part in range(3):
            picks = jnp.where(source == target + part * count, 1.0, picks)
        picks = picks.astype(jnp.bfloat16)

        def one(block):
            start = pl.multiple_of(block * LINES, 8)
            lines = feats[pl.ds(start, 32), :].astype(jnp.bfloat16)
            wide = lax.dot_general(
                lines, picks, (((0,), (0,)), ((), ())), preferred_element_type=jnp.float32
            )
            for f in range(count):
                for piece in range(PIECES):
                    rowbs[slot][(block * count + f) * PIECES + piece] = wide[
                        piece * ROWS : (piece + 1) * ROWS, f * TILE : (f + 1) * TILE
                    ]

        def some(step, carry):
            for part in range(together):
                one(step * together + part)
            return carry

        together = SPREAD if own % SPREAD == 0 else 1
        lax.fori_loop(0, own // together, some, 0)

    def start_state(slot):
        zero = jnp.zeros((ROWS, TILE), jnp.float32)
        row = jnp.zeros((1, TILE), jnp.float32)
        return tuple(zero for _ in range(lams_of(slot))) + (row, row)

    def tiles(slot, phase, first, last, state):
        lams = lambda_list(slot)
        softs = [2.0 - lam for lam in lams]
        count = fields_of(slot)
        unroll = max(u for u in (1, 2, UNROLL, 5, 8, 10) if (last - first) % u == 0)

        def pair_sum(pair, state):
            word = order[slot, pair]
            same = (word & 1).astype(jnp.float32)
            mine = jnp.clip((word >> 1) & (2**row_bits - 1), 0, own - 1) * (count * PIECES)
            index = jnp.clip((word >> (1 + row_bits)) & (2**index_bits - 1), 0, near * unit - 1)
            step_of = word >> (1 + row_bits + index_bits)
            col = [bufs[slot][0][index, f] for f in range(FIELDS)]
            if phase > 0:
                far = jnp.clip(jnp.where(step_of < near, 0, index), 0, unit - 1)
                for part in range(1, phase + 1):
                    here = step_of == near + part - 1
                    col = [
                        jnp.where(here, bufs[slot][part][far, f], col[f]) for f in range(FIELDS)
                    ]
            fields = [jnp.broadcast_to(col[f], (ROWS, TILE)) for f in range(3)]
            charge_col = col[3]
            depth_col = col[4]
            size_col = jnp.broadcast_to(1.0 / col[5], (ROWS, TILE))
            sum_disp = [None] * len(lams)
            sum_coul = [None] * len(lams)
            for piece in range(PIECES):
                wide = [rowbs[slot][mine + (f * PIECES + piece)] for f in range(count)]
                dx = wide[0] - fields[0]
                dy = wide[1] - fields[1]
                dz = wide[2] - fields[2]
                r2 = dx * dx + dy * dy + dz * dz
                scaled = r2 * (wide[5] * size_col)
                cube = scaled * scaled * scaled
                for k in range(len(lams)):
                    inverse = 1.0 / (cube + wide[FIELDS + k])
                    disp = inverse * (inverse - wide[4])
                    coul = wide[3] * lax.rsqrt(r2 + softs[k])
                    if piece == 0:
                        sum_disp[k], sum_coul[k] = disp, coul
                    else:
                        sum_disp[k] = sum_disp[k] + disp
                        sum_coul[k] = sum_coul[k] + coul
            depth_four = 4.0 * depth_col
            totals = [
                state[k] + (sum_disp[k] * depth_four + sum_coul[k] * charge_col)
                for k in range(len(lams))
            ]
            return tuple(totals) + (
                state[-2] + same * (depth_col * depth_col),
                state[-1] + same * (charge_col * charge_col),
            )

        def some(step, state):
            for part in range(unroll):
                state = pair_sum(first + step * unroll + part, state)
            return state

        return lax.fori_loop(0, (last - first) // unroll, some, state)

    def close(slot, state):
        sums = []
        for k, lam in enumerate(lambda_list(slot)):
            core = jnp.full((1, TILE), 1.0 - 0.5 * lam, jnp.float32)
            soft = jnp.full((1, TILE), 2.0 - lam, jnp.float32)
            inverse = 1.0 / core
            own_pairs = state[-2] * (4.0 * inverse * (inverse - 1.0)) + state[-1] * lax.rsqrt(soft)
            line = jnp.sum(state[k], axis=0, keepdims=True) - own_pairs
            sums.append(jnp.sum(line, axis=1, keepdims=True) * lam)
        if two_ends and slot == 1:
            sums = [sums[0], jnp.where(win == 0, sums[0], sums[1]), sums[1]]
        return sums

    for slot in range(run):
        open_sends(slot)
    ordered = pltpu.make_async_copy(words, order, order_sem)
    ordered.start()
    spread(0)
    known = questions()
    known.wait()
    answer(0, 0)
    if dim_z > 1:
        answer(0, 1)
    for slot in range(1, run):
        answer(slot, 0)
    for slot in range(1, run):
        spread(slot)

    shares = []
    lowers = []
    for wl in range(run):
        window = win * run + wl
        odd = (window + parity[0]) & 1
        lower = window - odd
        threshold = thresholds[0]
        for v in range(1, windows):
            threshold = jnp.where(lower == v, thresholds[v], threshold)
        drawn = ((threshold + parity[0]) & 1073741823) + 1
        share = jnp.full((ROWS, TILE), drawn, jnp.int32).astype(jnp.float32) * (1.0 / 1073741824.0)
        shares.append(-jnp.log(share))
        lowers.append(lower)

    for step in range(2, dim_z):
        answer(0, step)
        if run > 1:
            answer(1, step - 1)
    ordered.wait()
    ends = phases_of(dims, groups, listed)

    def complete(slot, phase):
        for step in range(near) if phase == 0 else [near + phase - 1]:
            answered(slot, step)

    later = []
    for slot in range(1, run):
        first_step = dim_z - 1 if slot == 1 and dim_z > 2 else 1
        later += [functools.partial(answer, slot, step) for step in range(first_step, dim_z)]
    turns = [(slot, phase) for slot in range(run) for phase in range(len(ends))]
    if run == 2 and len(ends) > 2:
        turns.sort(key=lambda turn: (turn[1] + HEAD * turn[0], turn[0]))
    states = [start_state(slot) for slot in range(run)]
    for slot, phase in turns:
        complete(slot, phase)
        if slot == 0 and phase == len(ends) - 1:
            for partner in partners:
                pl.semaphore_signal(ready, inc=1, device_id=partner, device_id_type=MESH)
        first = ends[phase - 1] if phase else 0
        if ends[phase] > first:
            states[slot] = tiles(slot, phase, first, ends[phase], states[slot])
        if later:
            later.pop(0)()
            while slot == 0 and phase == len(ends) - 1 and later:
                later.pop(0)()
    partial = [close(slot, states[slot]) for slot in range(run)]

    lane = lax.broadcasted_iota(jnp.int32, (1, TILE), 1)
    line = jnp.zeros((1, TILE), jnp.float32)
    for slot in range(run):
        place = (win * run + window_of(slot)) * 3
        for k in range(3):
            line = jnp.where(lane == place + k, partial[slot][k], line)
    red[me] = line
    for _ in partners:
        pl.semaphore_wait(ready, 1)
    everyone = wins * groups
    for step in range(dim_z - 1, -1, -1):
        for dy, dx, other_win in itertools.product(*map(backward, (dim_y, dim_x, wins))):
            if step or dy or dx or other_win:
                target = ((win + other_win) % wins, group_at(plane_to(step), dy, dx))
                pltpu.make_async_remote_copy(
                    src_ref=red.at[me],
                    dst_ref=red.at[me],
                    send_sem=red_send.at[0],
                    recv_sem=red_recv.at[0],
                    device_id=target,
                    device_id_type=MESH,
                ).start()
    for copy in sent + asking:
        copy.wait_send()
    rest = pltpu.make_async_remote_copy(
        src_ref=red.at[pl.ds(0, everyone - 1)],
        dst_ref=red.at[pl.ds(0, everyone - 1)],
        send_sem=red_send.at[0],
        recv_sem=red_recv.at[0],
        device_id=((win + 1) % wins, (grp + 1) % groups),
        device_id_type=MESH,
    )
    rest.wait_recv()
    rest.wait_send()
    scale = 1.0 / (listed * groups * TILE * TILE)
    total = jnp.sum(red[0:everyone], axis=0) * scale
    energy = [
        [jnp.sum(jnp.where(lane == v * 3 + k, total, 0.0)) for k in range(3)]
        for v in range(windows)
    ]
    ups = [e[2] - e[1] for e in energy]
    downs = [e[0] - e[1] for e in energy]
    rows = lax.broadcasted_iota(jnp.int32, (ROWS, TILE), 0)
    lanes = lax.broadcasted_iota(jnp.int32, (ROWS, TILE), 1)
    cell = rows * TILE + lanes
    result = jnp.zeros((ROWS, TILE), jnp.float32)
    for wl in range(run):
        window = win * run + wl
        for k in range(3):
            value = energy[wl][k]
            for part in range(1, wins):
                value = jnp.where(win == part, energy[part * run + wl][k], value)
            result = jnp.where(cell == wl * TILE + k, value, result)
        profile = jnp.float32(0.0)
        change = jnp.float32(0.0)
        for v in range(windows):
            profile = profile + jnp.where(v < window, ups[v], 0.0)
            change = change + jnp.where(lowers[wl] == v, ups[v], 0.0)
            change = change + jnp.where(lowers[wl] + 1 == v, downs[v], 0.0)
        result = jnp.where(cell == (run + 1) * TILE + wl, profile, result)
        partner = jnp.logical_and(lowers[wl] >= 0, lowers[wl] + 1 < windows)
        margin = shares[wl] - inverse_temp[0] * change
        margin = jnp.where(partner, margin, 0.0)
        result = jnp.where(cell == run * TILE + wl, margin, result)
    out[...] = result


def finish(run, total, out_energy, out_margin, out_profile):
    out_energy[...] = total[0:run, 0:3]
    out_margin[...] = total[run, 0:run]
    out_profile[...] = total[run + 1, 0:run]


def per_device(dims, atom_table, row_blocks, col_blocks, lambdas, inverse_temp, parity, thresholds):
    run, fields, atoms = atom_table.shape
    wins = lax.axis_size("win")
    groups = lax.axis_size("grp")
    own = atoms // TILE
    listed = row_blocks.shape[1]
    cfg = (run, wins, groups, own, listed, dims)
    hbm = pl.BlockSpec(memory_space=pltpu.HBM)
    vmem = pl.BlockSpec(memory_space=pltpu.VMEM)
    smem = pl.BlockSpec(memory_space=pltpu.SMEM)
    own_pad = -(-own // 8) * 8
    counts = [9] * run
    if wins == 2 and run == 2:
        counts[1] = 8
    near = near_steps(dims)
    plane = dims[1] * dims[2]
    slots = slots_of(groups, listed)
    unit = plane * slots
    width = -(-plane * dims[0] * slots // TILE) * TILE
    answers = max(1, dims[0] * (plane - 1) * slots)
    scratch = []
    for _ in range(run):
        for planes in [near] + [1] * (dims[0] - near):
            scratch.append(pltpu.VMEM((planes * unit, FIELDS, 1, TILE), jnp.float32))
    scratch += [pltpu.VMEM((own, FIELDS, 1, TILE), jnp.float32) for _ in range(run * dims[0])]
    scratch += [pltpu.VMEM((own * count * PIECES, ROWS, TILE), jnp.float32) for count in counts]
    scratch += [
        pltpu.VMEM((run, FIELDS, own_pad, TILE), jnp.float32),
        pltpu.VMEM((LINES * (own_pad + 1), TILE), jnp.float32),
        pltpu.VMEM((wins * groups, 1, TILE), jnp.float32),
        pltpu.VMEM((run, listed), jnp.int32),
        pltpu.VMEM((run, listed), jnp.int32),
        pltpu.VMEM((run, listed), jnp.int32),
        pltpu.SMEM((run, listed), jnp.int32),
        pltpu.VMEM((run, answers, FIELDS, 1, TILE), jnp.float32),
        pltpu.VMEM((plane, run, 1, width), jnp.int32),
        pltpu.SMEM((plane, run, 1, width), jnp.int32),
        pltpu.SMEM((wins * run,), jnp.float32),
        pltpu.SMEM((wins * run,), jnp.int32),
        pltpu.SemaphoreType.DMA((2 * run,)),
        pltpu.SemaphoreType.DMA((4,)),
        pltpu.SemaphoreType.DMA((run, max(1, messages_of(dims)))),
        pltpu.SemaphoreType.DMA((run, dims[0], dims[1] * dims[2])),
        pltpu.SemaphoreType.DMA((1,)),
        pltpu.SemaphoreType.DMA((1,)),
        pltpu.SemaphoreType.REGULAR,
        pltpu.SemaphoreType.DMA,
        pltpu.SemaphoreType.DMA((plane,)),
        pltpu.SemaphoreType.DMA((plane,)),
        pltpu.SemaphoreType.DMA,
    ]
    table = jnp.transpose(atom_table.reshape(run, fields, own, TILE), (1, 2, 0, 3))
    total = pl.pallas_call(
        functools.partial(kernel, cfg),
        out_shape=jax.ShapeDtypeStruct((8, TILE), jnp.float32),
        in_specs=[hbm, hbm, hbm, hbm, smem, smem, hbm],
        out_specs=vmem,
        scratch_shapes=scratch,
        compiler_params=pltpu.CompilerParams(
            collective_id=0, has_side_effects=True, vmem_limit_bytes=LIMIT
        ),
    )(table, row_blocks, col_blocks, lambdas, inverse_temp, parity, thresholds)
    shapes = (
        jax.ShapeDtypeStruct((run, 3), jnp.float32),
        jax.ShapeDtypeStruct((run,), jnp.float32),
        jax.ShapeDtypeStruct((run,), jnp.float32),
    )
    return pl.pallas_call(
        functools.partial(finish, run),
        out_shape=shapes,
        in_specs=[vmem],
        out_specs=(vmem, vmem, vmem),
        compiler_params=pltpu.CompilerParams(vmem_limit_bytes=1024 * 1024),
    )(total)


def solution(mesh):
    return jax.shard_map(
        functools.partial(per_device, grid_of(mesh)),
        mesh=mesh,
        in_specs=(P("win", None, "grp"), P("win", "grp"), P("win", "grp"), P(), P(), P(), P()),
        out_specs=(P("win", None), P("win"), P("win")),
        check_vma=False,
    )
```
